512 devices in a mesh: slab: 512 (over z, x, y, core).
Axes of the slice: x: 4, y: 8, z: 8, core: 2. Of those that a mesh axis runs over, the one named last changes fastest.
Arguments:
- start_vectors: float32 [2, 512, 256, 256], P(None, 'slab'), may hold values from -6 to 6
- levels: int32 [512, 256, 256], P('slab'), may hold values from 0 to 15
- energies: float32 [16], replicated, may hold values from -4 to 4
Outputs:
- cheb_field: float32 [2, 512, 256, 256], P(None, 'slab')
- lanczos_diag: float32 [2, 8], replicated
- lanczos_off: float32 [2, 7], replicated
- moments: float32 [2, 6], replicated
The draws below stay inside these ranges and needn't reach their ends.
All inputs are finite; a program needn't handle non-finite values.
Results may differ from the reference program's by a relative error of at most 0.0001.
Values sent between devices are 32-bit elements; how exact they have to be, the bound alone decides.
A program may use at most 64 MiB of HBM per device.

```python
import jax
import jax.numpy as jnp
from jax import lax

NY = 256
NX = 256
VECS = 2
LANCZOS = 8
LEVELS = 16
NZ = 512


def place_ends(entries, stream_key, low, largest):
    shape = entries.shape
    index_at = [jax.random.randint(jax.random.fold_in(stream_key, axis), (), 0, shape[axis]) for axis in range(len(shape))]
    entries = entries.at[tuple(index_at)].set(low)
    longest = shape.index(max(shape))
    index_at[longest] = (index_at[longest] + 1) % shape[longest]
    return entries.at[tuple(index_at)].set(largest)


def shard_levels(stream_key, shape, cuts, least, largest):
    loudness = 1.0
    for position, blocks in cuts:
        heights = jax.random.uniform(jax.random.fold_in(jax.random.fold_in(stream_key, 6), position), (blocks,), jnp.float32, least / len(cuts), largest / len(cuts))
        loudness = loudness * jnp.repeat(jnp.exp(heights), shape[position] // blocks).reshape((-1,) + (1,) * (len(shape) - 1 - position))
    return loudness


def normal_values(stream_key, extent, spread, most, shards=(), held_as=jnp.bfloat16):
    array = spread * jax.random.normal(stream_key, extent, jnp.float32)
    if shards:
        array = array * shard_levels(stream_key, extent, shards, -0.22, 0.18)
    return jnp.clip(array, -most, most).astype(held_as)


def setup_inputs(seed: int = 0) -> dict:
    arg_keys = jax.random.split(jax.random.key(seed), 4)
    return {
        "start_vectors": normal_values(arg_keys[0], (VECS, NZ, NY, NX), 1.0, 6.0, ((1, 512),), jnp.float32),
        "levels": place_ends(jax.random.randint(arg_keys[1], (NZ, NY, NX), 0, LEVELS), jax.random.fold_in(arg_keys[1], 1), 0, LEVELS - 1).astype(jnp.int32),
        "energies": jnp.clip(jax.random.uniform(arg_keys[2], (LEVELS,), jnp.float32, -4.0, 4.0), -4.0, 4.0),
    }


def hamiltonian(field, onsite):
    beside = jnp.roll(field, 1, 1) + jnp.roll(field, -1, 1)
    beside = beside + jnp.roll(field, 1, 2) + jnp.roll(field, -1, 2)
    beside = beside + jnp.roll(field, 1, 3) + jnp.roll(field, -1, 3)
    return onsite[None] * field - beside

def inner(first, second):
    return lax.optimization_barrier(jnp.sum(first * second, axis=(1, 2, 3)))

def expand(values):
    return values[:, None, None, None]

def reference(start_vectors, levels, energies):
    onsite = jnp.take(energies, levels, axis=0)
    norm0 = inner(start_vectors, start_vectors)
    vector = start_vectors / expand(jnp.sqrt(norm0))
    previous = jnp.zeros_like(vector)
    beta_prev = jnp.zeros((VECS,), jnp.float32)
    alphas = []
    betas = []
    for step in range(LANCZOS):
        work = hamiltonian(vector, onsite) - expand(beta_prev) * previous
        alpha = inner(vector, work)
        alphas.append(alpha)
        if step < LANCZOS - 1:
            work = work - expand(alpha) * vector
            beta = jnp.sqrt(inner(work, work))
            betas.append(beta)
            previous, vector, beta_prev = (vector, work / expand(beta), beta)
    diag = jnp.stack(alphas, axis=1)
    offd = jnp.stack(betas, axis=1)
    zero_col = jnp.zeros((VECS, 1), jnp.float32)
    left = jnp.concatenate([zero_col, offd], axis=1)
    right = jnp.concatenate([offd, zero_col], axis=1)
    emin = lax.optimization_barrier(jnp.min(diag - left - right, axis=1))
    emax = lax.optimization_barrier(jnp.max(diag + left + right, axis=1))
    center = expand((emax + emin) * 0.5)
    half = expand(0.55 * (emax - emin))

    def scaled(field):
        return (hamiltonian(field, onsite) - center * field) / half
    term0 = start_vectors
    term1 = scaled(term0)
    term2 = 2.0 * scaled(term1) - term0
    term3 = 2.0 * scaled(term2) - term1
    first = inner(term0, term1)
    moments = jnp.stack([first, inner(term0, term2), inner(term0, term3), 2.0 * inner(term2, term2) - norm0, 2.0 * inner(term3, term2) - first, 2.0 * inner(term3, term3) - norm0], axis=1) / norm0[:, None]
    return (term3, diag, offd, moments)
```

```python
import functools

import jax
import jax.numpy as jnp
from jax import lax
from jax.experimental import pallas as pl
from jax.experimental.pallas import tpu as pltpu
from jax.sharding import PartitionSpec as P

LANCZOS = 8
RING = 16
PARTS = 2
PAD = 8
FAR = 64


def two_sum(a, b):
    s = a + b
    t = s - a
    return s, (a - (s - t)) + (b - t)


def quick(a, b):
    s = a + b
    return s, b - (s - a)


def split(a):
    t = 4097.0 * a
    high = t - (t - a)
    return high, a - high


def two_prod(a, b):
    p = a * b
    ah, al = split(a)
    bh, bl = split(b)
    return p, ((ah * bh - p) + ah * bl + al * bh) + al * bl


def add(x, y):
    s, e = two_sum(x[0], y[0])
    return quick(s, e + (x[1] + y[1]))


def sub(x, y):
    return add(x, (-y[0], -y[1]))


def mul(x, y):
    p, e = two_prod(x[0], y[0])
    return quick(p, e + (x[0] * y[1] + x[1] * y[0]))


def scale(x, c):
    return x[0] * c, x[1] * c


def div(x, y):
    q = x[0] / y[0]
    p, e = two_prod(q, y[0])
    return quick(q, (((x[0] - p) - e) + (x[1] - q * y[1])) / y[0])


def coefficients(dots):
    count = len(dots)
    norm = dots[0]
    nu = [(norm[0] / norm[0], norm[0] * 0.0), div(dots[1], norm)]
    for k in range(2, count):
        nu.append(sub(scale(div(dots[k], norm), 2.0), nu[k % 2]))
    row, before = nu, None
    diag, square = [], []
    for k in range(LANCZOS):
        if k == 0:
            alpha = row[1]
        else:
            alpha = div(sub(scale(row[k + 1], 0.5), mul(square[-1], before[k])), row[k])
        diag.append(alpha)
        if k == LANCZOS - 1:
            break
        new = [None] * count
        for l in range(k + 1, count - 1 - k):
            x = sub(scale(add(row[l + 1], row[l - 1]), 0.5), mul(alpha, row[l]))
            new[l] = sub(x, mul(square[-1], before[l])) if k else x
        square.append(div(new[k + 1], row[k] if k == 0 else scale(row[k], 2.0)))
        before, row = row, new
    return [x[0] for x in nu], [x[0] for x in diag], [jnp.sqrt(x[0]) for x in square]


def chebyshev(diag, offd, nu, centre, width):
    left = [None] + offd
    right = offd + [None]
    low, high = None, None
    for a, b, c in zip(diag, left, right):
        reach = b if c is None else c if b is None else b + c
        low = a - reach if low is None else jnp.minimum(low, a - reach)
        high = a + reach if high is None else jnp.maximum(high, a + reach)
    inv = 1.0 / (0.55 * (high - low))
    al = width * inv
    be = (centre - 0.5 * (high + low)) * inv
    p, q, r = 2.0 * be * be + al * al - 1.0, 4.0 * al * be, al * al
    first = [be, al]
    second = [p, q, r]
    third = [2.0 * be * p + al * q - be, 2.0 * be * q + al * (2.0 * p + r) - al, 2.0 * be * r + al * q, al * r]

    def dot(f, g):
        total = None
        for i, x in enumerate(f):
            for j, y in enumerate(g):
                term = (x * y) * (0.5 * (nu[i + j] + nu[abs(i - j)]))
                total = term if total is None else total + term
        return total

    start = [nu[0]]
    m1 = dot(start, first)
    moments = [
        m1,
        dot(start, second),
        dot(start, third),
        2.0 * dot(second, second) - 1.0,
        2.0 * dot(third, second) - m1,
        2.0 * dot(third, third) - 1.0,
    ]
    return third, moments


def kernel(
    count, energies, start, levels, cheb, diag_out, offd_out, moments_out,
    field, halo, level, onsite, near_part, far_part, mine,
    load_sem, send_sem, recv_sem, red_send, red_recv,
):
    me = lax.axis_index("slab")
    member = lax.rem(me, RING)
    ring = me // RING
    base = me - member
    rings = count // RING
    vecs, _, height, lanes = start.shape
    rows = height // PARTS
    mesh_id = pl.DeviceIdType.MESH
    ahead = lax.rem(me + 1, count)
    behind = lax.rem(me + count - 1, count)

    loads = [
        pltpu.make_async_copy(start.at[v, 0], field.at[0, v, pl.ds(PAD, height)], load_sem.at[v]) for v in range(vecs)
    ]
    loads.append(pltpu.make_async_copy(levels.at[0], level, load_sem.at[vecs]))
    for copy in loads:
        copy.start()

    def peer(i):
        return base + lax.rem(member + i, RING)

    def far(i):
        return lax.rem(me + i * RING, count)

    barrier = pltpu.get_barrier_semaphore()

    def greet(to):
        pl.semaphore_signal(barrier, inc=1, device_id=(to,), device_id_type=mesh_id)

    def greet_peer(i, carry):
        greet(peer(i))
        return carry

    def greet_far(i, carry):
        greet(far(i))
        return carry

    greet(ahead)
    greet(behind)
    lax.fori_loop(1, RING, greet_peer, 0)
    lax.fori_loop(1, rings, greet_far, 0)

    values = [energies[i] for i in range(energies.shape[0])]
    mean = sum(values[1:], values[0]) * (1.0 / len(values))
    spread = [(x - mean) * (x - mean) for x in values]
    spread = sum(spread[1:], spread[0]) * (1.0 / len(values))
    width = 2.0 * jnp.sqrt(jnp.full((1, 128), spread + 6.0, jnp.float32))
    inv_width = 1.0 / width
    inv_wide = jnp.concatenate([inv_width] * (lanes // 128), axis=1)

    loads[vecs].wait()
    for at in range(0, height, 64):
        ids = level[at : at + 64]
        energy = jnp.full(ids.shape, values[0] - mean, jnp.float32)
        for i in range(1, len(values)):
            energy = jnp.where(ids == i, values[i] - mean, energy)
        onsite[at : at + 64] = energy * inv_wide

    pl.semaphore_wait(barrier, 2 + RING - 1 + rings - 1)

    def part_copy(k, v, h, side):
        to = ahead if side == 0 else behind
        at = h * rows
        return pltpu.make_async_remote_copy(
            src_ref=field.at[k, v, pl.ds(PAD + at, rows)],
            dst_ref=halo.at[k, side, v, pl.ds(at, rows)],
            send_sem=send_sem.at[k, side, v, h], recv_sem=recv_sem.at[k, side, v, h],
            device_id=(to,), device_id_type=mesh_id,
        )

    def sides(k, h):
        if k < LANCZOS - 1:
            return (0, 1)
        return (0,) if h < PARTS // 2 else (1,)

    sent = []

    def send(k, v, h):
        for side in sides(k, h):
            copy = part_copy(k, v, h, side)
            copy.start()
            sent.append(copy)

    for v in range(vecs):
        loads[v].wait()
        for h in range(PARTS):
            send(0, v, h)
        field[0, v, 0:PAD] = field[0, v, height : height + PAD]
        field[0, v, PAD + height :] = field[0, v, PAD : 2 * PAD]

    def tile_sum(x):
        total = x[0:8]
        for i in range(8, rows, 8):
            total = total + x[i : i + 8]
        return total

    sums = {}

    def note(d, v, x):
        x = tile_sum(x)
        sums[d, v] = sums[d, v] + x if (d, v) in sums else x

    def unit(k, v, h):
        at = h * rows
        big = field[k, v, at : at + rows + 2 * PAD]
        deep = rows + 2 * PAD
        near = (pltpu.roll(big, 1, 0) + pltpu.roll(big, deep - 1, 0))[PAD : PAD + rows]
        here = big[PAD : PAD + rows]
        near = near + pltpu.roll(here, 1, 1) + pltpu.roll(here, lanes - 1, 1)
        for side in sides(k, h):
            part_copy(k, v, h, side).wait_recv()
        if k < LANCZOS - 1:
            near = near + (halo[k, 0, v, at : at + rows] + halo[k, 1, v, at : at + rows])
        else:
            near = near + 2.0 * halo[k, sides(k, h)[0], v, at : at + rows]
        new = onsite[at : at + rows] * here - inv_wide * near
        if k:
            new = 2.0 * new - field[k - 1, v, PAD + at : PAD + at + rows]
        if k < LANCZOS - 1:
            field[k + 1, v, PAD + at : PAD + at + rows] = new
            if h == 0:
                field[k + 1, v, PAD + height :] = new[0:PAD]
            if h == PARTS - 1:
                field[k + 1, v, 0:PAD] = new[rows - PAD :]
            send(k + 1, v, h)
        note(2 * k, v, here * here)
        note(2 * k + 1, v, here * new)

    for k in range(LANCZOS):
        for v in range(vecs):
            for h in range(PARTS):
                unit(k, v, h)

    lane = lax.broadcasted_iota(jnp.int32, (vecs, 128), 1)
    line = lax.broadcasted_iota(jnp.int32, (vecs, 128), 0)
    tile = jnp.zeros((vecs, 128), jnp.float32)
    for d in range(2 * LANCZOS):
        for v in range(vecs):
            whole = jnp.sum(jnp.sum(sums[d, v], axis=0, keepdims=True), axis=1, keepdims=True)
            tile = jnp.where((lane == d) & (line == v), whole, tile)

    def exchange(leg, slots, index, size, target, tile):
        mine[leg] = tile
        slots[index] = tile

        def body(i, carry):
            pltpu.make_async_remote_copy(
                src_ref=mine.at[leg], dst_ref=slots.at[index],
                send_sem=red_send.at[leg], recv_sem=red_recv.at[leg],
                device_id=(target(i),), device_id_type=mesh_id,
            ).start()
            return carry

        lax.fori_loop(1, size, body, 0)
        rest = slots.at[pl.ds(0, size - 1)]
        pltpu.make_async_copy(rest, rest, red_recv.at[leg]).wait()

    exchange(0, near_part, member, RING, peer, tile)
    pairs = [two_sum(near_part[i], near_part[i + 1]) for i in range(0, RING, 2)]
    while len(pairs) > 1:
        pairs = [add(x, y) for x, y in zip(pairs[::2], pairs[1::2])]
    high, low = pairs[0]
    tile = jnp.where(lane < FAR, high, pltpu.roll(low, FAR, 1))
    exchange(1, far_part, ring, rings, far, tile)
    pairs = []
    for i in range(rings):
        both = far_part[i]
        pairs.append((both, pltpu.roll(both, FAR, 1)))
    while len(pairs) > 1:
        pairs = [add(x, y) for x, y in zip(pairs[::2], pairs[1::2])]
    high, low = pairs[0]

    def pick(x, d):
        return jnp.broadcast_to(x[:, d : d + 1], (vecs, 128))

    dots = [(pick(high, d), pick(low, d)) for d in range(2 * LANCZOS)]
    nu, diag, offd = coefficients(dots)
    diag = [width * a + mean for a in diag]
    offd = [width * b for b in offd]
    third, moments = chebyshev(diag, offd, nu, mean, width)

    for v in range(vecs):
        weights = [jnp.concatenate([x[v : v + 1]] * (lanes // 128), axis=1) for x in third]
        total = weights[0] * field[0, v, PAD : PAD + height]
        for k in range(1, len(weights)):
            total = total + weights[k] * field[k, v, PAD : PAD + height]
        cheb[v, 0] = total

    for ref, items in ((diag_out, diag), (offd_out, offd), (moments_out, moments)):
        at = lax.broadcasted_iota(jnp.int32, ref.shape, 1)
        value = jnp.zeros(ref.shape, jnp.float32)
        for i, item in enumerate(items):
            value = jnp.where(at == i, item[:, : ref.shape[1]], value)
        ref[...] = value

    for copy in sent:
        copy.wait_send()
    for leg, (slots, size) in enumerate(((near_part, RING), (far_part, rings))):
        rest = slots.at[pl.ds(0, size - 1)]
        pltpu.make_async_copy(rest, rest, red_send.at[leg]).wait()


def shards(count, start_vectors, levels, energies):
    vecs, _, height, lanes = start_vectors.shape
    rings = count // RING
    f32 = jnp.float32
    vmem = pl.BlockSpec(memory_space=pltpu.VMEM)
    anywhere = pl.BlockSpec(memory_space=pl.ANY)
    dma = pltpu.SemaphoreType.DMA
    return pl.pallas_call(
        functools.partial(kernel, count),
        out_shape=(
            jax.ShapeDtypeStruct(start_vectors.shape, f32),
            jax.ShapeDtypeStruct((vecs, LANCZOS), f32),
            jax.ShapeDtypeStruct((vecs, LANCZOS - 1), f32),
            jax.ShapeDtypeStruct((vecs, 6), f32),
        ),
        in_specs=[pl.BlockSpec(memory_space=pltpu.SMEM), anywhere, anywhere],
        out_specs=(vmem,) * 4,
        scratch_shapes=[
            pltpu.VMEM((LANCZOS, vecs, height + 2 * PAD, lanes), f32),
            pltpu.VMEM((LANCZOS, 2, vecs, height, lanes), f32),
            pltpu.VMEM((height, lanes), jnp.int32),
            pltpu.VMEM((height, lanes), f32),
            pltpu.VMEM((RING, vecs, 128), f32),
            pltpu.VMEM((rings, vecs, 128), f32),
            pltpu.VMEM((2, vecs, 128), f32),
            dma((vecs + 1,)),
            dma((LANCZOS, 2, vecs, PARTS)),
            dma((LANCZOS, 2, vecs, PARTS)),
            dma((2,)),
            dma((2,)),
        ],
        compiler_params=pltpu.CompilerParams(
            collective_id=0, has_side_effects=True, vmem_limit_bytes=67043328
        ),
    )(energies, start_vectors, levels)


def solution(mesh):
    in_specs = (P(None, "slab", None, None), P("slab", None, None), P())
    out_specs = (P(None, "slab", None, None), P(), P(), P())
    return jax.shard_map(
        functools.partial(shards, mesh.shape["slab"]),
        mesh=mesh, in_specs=in_specs, out_specs=out_specs, check_vma=False,
    )
```

```python
import functools

import jax
import jax.numpy as jnp
from jax import lax
from jax.experimental import pallas as pl
from jax.experimental.pallas import tpu as pltpu
from jax.sharding import PartitionSpec as P

LANCZOS = 8
RING = 16
PARTS = 4
PAD = 8
FAR = 64
RETURNED = 4
GAP = 6


def two_sum(a, b):
    s = a + b
    t = s - a
    return s, (a - (s - t)) + (b - t)


def quick(a, b):
    s = a + b
    return s, b - (s - a)


def split(a):
    t = 4097.0 * a
    high = t - (t - a)
    return high, a - high


def two_prod(a, b):
    p = a * b
    ah, al = split(a)
    bh, bl = split(b)
    return p, ((ah * bh - p) + ah * bl + al * bh) + al * bl


def add(x, y):
    s, e = two_sum(x[0], y[0])
    return quick(s, e + (x[1] + y[1]))


def sub(x, y):
    return add(x, (-y[0], -y[1]))


def mul(x, y):
    p, e = two_prod(x[0], y[0])
    return quick(p, e + (x[0] * y[1] + x[1] * y[0]))


def scale(x, c):
    return x[0] * c, x[1] * c


def div(x, y):
    q = x[0] / y[0]
    p, e = two_prod(q, y[0])
    return quick(q, (((x[0] - p) - e) + (x[1] - q * y[1])) / y[0])


def coefficients(dots):
    count = len(dots)
    norm = dots[0]
    nu = [(norm[0] / norm[0], norm[0] * 0.0), div(dots[1], norm)]
    for k in range(2, count):
        nu.append(sub(scale(div(dots[k], norm), 2.0), nu[k % 2]))
    row, before = nu, None
    diag, square = [], []
    for k in range(LANCZOS):
        if k == 0:
            alpha = row[1]
        else:
            alpha = div(sub(scale(row[k + 1], 0.5), mul(square[-1], before[k])), row[k])
        diag.append(alpha)
        if k == LANCZOS - 1:
            break
        new = [None] * count
        for l in range(k + 1, count - 1 - k):
            x = sub(scale(add(row[l + 1], row[l - 1]), 0.5), mul(alpha, row[l]))
            new[l] = sub(x, mul(square[-1], before[l])) if k else x
        square.append(div(new[k + 1], row[k] if k == 0 else scale(row[k], 2.0)))
        before, row = row, new
    return [x[0] for x in nu], [x[0] for x in diag], [jnp.sqrt(x[0]) for x in square]


def chebyshev(diag, offd, nu, centre, width):
    left = [None] + offd
    right = offd + [None]
    low, high = None, None
    for a, b, c in zip(diag, left, right):
        reach = b if c is None else c if b is None else b + c
        low = a - reach if low is None else jnp.minimum(low, a - reach)
        high = a + reach if high is None else jnp.maximum(high, a + reach)
    inv = 1.0 / (0.55 * (high - low))
    al = width * inv
    be = (centre - 0.5 * (high + low)) * inv
    p, q, r = 2.0 * be * be + al * al - 1.0, 4.0 * al * be, al * al
    first = [be, al]
    second = [p, q, r]
    third = [2.0 * be * p + al * q - be, 2.0 * be * q + al * (2.0 * p + r) - al, 2.0 * be * r + al * q, al * r]

    def dot(f, g):
        total = None
        for i, x in enumerate(f):
            for j, y in enumerate(g):
                term = (x * y) * (0.5 * (nu[i + j] + nu[abs(i - j)]))
                total = term if total is None else total + term
        return total

    start = [nu[0]]
    m1 = dot(start, first)
    moments = [
        m1,
        dot(start, second),
        dot(start, third),
        2.0 * dot(second, second) - 1.0,
        2.0 * dot(third, second) - m1,
        2.0 * dot(third, third) - 1.0,
    ]
    return third, moments


def kernel(
    count, energies, start, levels, terms, sums_out, table,
    field, halo, level, onsite, near_part, mine,
    load_sem, send_sem, recv_sem, last_sem, red_send, red_recv, known,
):
    me = lax.axis_index("slab")
    member = lax.rem(me, RING)
    ring = me // RING
    base = me - member
    rings = count // RING
    vecs, _, height, lanes = start.shape
    rows = height // PARTS
    mesh_id = pl.DeviceIdType.MESH

    def away(distance):
        return lax.rem(me + distance, count), lax.rem(me + count - distance, count)

    ahead, behind = away(1)

    def signal(sem, to):
        pl.semaphore_signal(sem, inc=1, device_id=(to,), device_id_type=mesh_id)

    barrier = pltpu.get_barrier_semaphore()
    for to in (ahead, behind):
        signal(barrier, to)
    loads = [
        pltpu.make_async_copy(start.at[v, 0], field.at[0, v, pl.ds(PAD, height)], load_sem.at[v]) for v in range(vecs)
    ]
    loads.append(pltpu.make_async_copy(levels.at[0], level, load_sem.at[vecs]))
    for copy in loads:
        copy.start()

    def peer(i):
        return base + lax.rem(member + i, RING)

    def far(i):
        return lax.rem(me + i * RING, count)

    rounds = (count // 2).bit_length() - 1

    def spread(i):
        if i:
            pl.semaphore_wait(known.at[i - 1], 2)
        if i < rounds:
            for to in away(2**i):
                signal(known.at[i], to)

    def part_copy(k, v, h, side):
        to = ahead if side == 0 else behind
        at = h * rows
        sender = last_sem.at[side] if k == LANCZOS - 1 else send_sem.at[side]
        return pltpu.make_async_remote_copy(
            src_ref=field.at[k, v, pl.ds(PAD + at, rows)],
            dst_ref=halo.at[k, side, v, pl.ds(at, rows)],
            send_sem=sender, recv_sem=recv_sem.at[k % 2, side, v, h],
            device_id=(to,), device_id_type=mesh_id,
        )

    def sides(k, h):
        if k < LANCZOS - 1:
            return (0, 1)
        return (0,) if h < PARTS // 2 else (1,)

    def send(k, v, h):
        for side in sides(k, h):
            part_copy(k, v, h, side).start()

    pl.semaphore_wait(barrier, 2)
    for v in range(vecs):
        loads[v].wait()
        for h in range(PARTS):
            send(0, v, h)

    values = [energies[i] for i in range(energies.shape[0])]
    mean = sum(values[1:], values[0]) * (1.0 / len(values))
    spread_of = [(x - mean) * (x - mean) for x in values]
    spread_of = sum(spread_of[1:], spread_of[0]) * (1.0 / len(values))
    width = 2.0 * jnp.sqrt(jnp.full((1, 128), spread_of + 6.0, jnp.float32))
    inv_width = 1.0 / width
    inv_wide = jnp.concatenate([inv_width] * (lanes // 128), axis=1)
    table[0:1] = width
    table[1:2] = jnp.full((1, 128), mean, jnp.float32)

    loads[vecs].wait()
    for at in range(0, height, 64):
        ids = level[at : at + 64]
        energy = jnp.full(ids.shape, values[0] - mean, jnp.float32)
        for i in range(1, len(values)):
            energy = jnp.where(ids == i, values[i] - mean, energy)
        onsite[at : at + 64] = energy * inv_wide
    for v in range(vecs):
        field[0, v, 0:PAD] = field[0, v, height : height + PAD]
        field[0, v, PAD + height :] = field[0, v, PAD : 2 * PAD]
        terms[0, v] = field[0, v, PAD : PAD + height]

    def tile_sum(x):
        total = x[0:8]
        for i in range(8, rows, 8):
            total = total + x[i : i + 8]
        return total

    sums = {}

    def note(d, v, x):
        x = tile_sum(x)
        sums[d, v] = sums[d, v] + x if (d, v) in sums else x

    def unit(k, v, h):
        at = h * rows
        big = field[k, v, at : at + rows + 2 * PAD]
        deep = rows + 2 * PAD
        near = (pltpu.roll(big, 1, 0) + pltpu.roll(big, deep - 1, 0))[PAD : PAD + rows]
        here = big[PAD : PAD + rows]
        near = near + pltpu.roll(here, 1, 1) + pltpu.roll(here, lanes - 1, 1)
        for side in sides(k, h):
            part_copy(k, v, h, side).wait_recv()
        if k < LANCZOS - 1:
            near = near + (halo[k, 0, v, at : at + rows] + halo[k, 1, v, at : at + rows])
        else:
            near = near + 2.0 * halo[k, sides(k, h)[0], v, at : at + rows]
        new = onsite[at : at + rows] * here - inv_wide * near
        if k:
            new = 2.0 * new - field[k - 1, v, PAD + at : PAD + at + rows]
        if k < LANCZOS - 1:
            field[k + 1, v, PAD + at : PAD + at + rows] = new
            if h == 0:
                field[k + 1, v, PAD + height :] = new[0:PAD]
            if h == PARTS - 1:
                field[k + 1, v, 0:PAD] = new[rows - PAD :]
            send(k + 1, v, h)
        if k + 1 < RETURNED:
            terms[k + 1, v, at : at + rows] = new
        note(2 * k, v, here * here)
        note(2 * k + 1, v, here * new)

    units = [(k, v, h) for k in range(LANCZOS) for v in range(vecs) for h in range(PARTS)]
    turn = 0
    for i, (k, v, h) in enumerate(units):
        if i == turn * GAP and turn <= rounds:
            spread(turn)
            turn += 1
        unit(k, v, h)
    while turn <= rounds:
        spread(turn)
        turn += 1

    lane = lax.broadcasted_iota(jnp.int32, (vecs, 128), 1)
    line = lax.broadcasted_iota(jnp.int32, (vecs, 128), 0)
    tile = jnp.zeros((vecs, 128), jnp.float32)
    for d in range(2 * LANCZOS):
        for v in range(vecs):
            whole = jnp.sum(jnp.sum(sums[d, v], axis=0, keepdims=True), axis=1, keepdims=True)
            tile = jnp.where((lane == d) & (line == v), whole, tile)

    def exchange(leg, slots, index, size, target, tile):
        mine[leg] = tile
        slots[index] = tile

        def body(i, carry):
            pltpu.make_async_remote_copy(
                src_ref=mine.at[leg], dst_ref=slots.at[index],
                send_sem=red_send.at[leg], recv_sem=red_recv.at[leg],
                device_id=(target(i),), device_id_type=mesh_id,
            ).start()
            return carry

        lax.fori_loop(1, size, body, 0)
        rest = slots.at[pl.ds(0, size - 1)]
        pltpu.make_async_copy(rest, rest, red_recv.at[leg]).wait()

    exchange(0, near_part, member, RING, peer, tile)
    pairs = [two_sum(near_part[i], near_part[i + 1]) for i in range(0, RING, 2)]
    while len(pairs) > 1:
        pairs = [add(x, y) for x, y in zip(pairs[::2], pairs[1::2])]
    high, low = pairs[0]
    tile = jnp.where(lane < FAR, high, pltpu.roll(low, FAR, 1))
    exchange(1, sums_out, ring, rings, far, tile)

    for side in range(2):
        whole = halo.at[pl.ds(0, LANCZOS - 1), 0]
        pltpu.make_async_copy(whole, whole, send_sem.at[side]).wait()
        half = halo.at[0, 0, pl.ds(0, vecs), pl.ds(0, height // 2)]
        pltpu.make_async_copy(half, half, last_sem.at[side]).wait()
    for leg, (slots, size) in enumerate(((near_part, RING), (sums_out, rings))):
        rest = slots.at[pl.ds(0, size - 1)]
        pltpu.make_async_copy(rest, rest, red_send.at[leg]).wait()


def finish(terms, parts, table, cheb, diag_out, offd_out, moments_out, result, out_sem):
    _, vecs, height, lanes = terms.shape
    width, mean = table[0:1], table[1:2]
    pairs = []
    for i in range(parts.shape[0]):
        both = parts[i]
        pairs.append((both, pltpu.roll(both, FAR, 1)))
    while len(pairs) > 1:
        pairs = [add(x, y) for x, y in zip(pairs[::2], pairs[1::2])]
    high, low = pairs[0]

    def pick(x, d):
        return jnp.broadcast_to(x[:, d : d + 1], (vecs, 128))

    dots = [(pick(high, d), pick(low, d)) for d in range(2 * LANCZOS)]
    nu, diag, offd = coefficients(dots)
    diag = [width * a + mean for a in diag]
    offd = [width * b for b in offd]
    third, moments = chebyshev(diag, offd, nu, mean, width)

    copies = []
    for v in range(vecs):
        weights = [jnp.concatenate([x[v : v + 1]] * (lanes // 128), axis=1) for x in third]
        total = weights[0] * terms[0, v]
        for k in range(1, len(weights)):
            total = total + weights[k] * terms[k, v]
        result[v] = total
        copies.append(pltpu.make_async_copy(result.at[v], cheb.at[v, 0], out_sem.at[v]))
        copies[-1].start()

    for ref, items in ((diag_out, diag), (offd_out, offd), (moments_out, moments)):
        at = lax.broadcasted_iota(jnp.int32, ref.shape, 1)
        value = jnp.zeros(ref.shape, jnp.float32)
        for i, item in enumerate(items):
            value = jnp.where(at == i, item[:, : ref.shape[1]], value)
        ref[...] = value
    for copy in copies:
        copy.wait()


def shards(count, start_vectors, levels, energies):
    vecs, _, height, lanes = start_vectors.shape
    rings = count // RING
    f32 = jnp.float32
    vmem = pl.BlockSpec(memory_space=pltpu.VMEM)
    anywhere = pl.BlockSpec(memory_space=pl.ANY)
    dma = pltpu.SemaphoreType.DMA
    terms, parts, table = pl.pallas_call(
        functools.partial(kernel, count),
        out_shape=(
            pltpu.VMEM((RETURNED, vecs, height, lanes), f32),
            pltpu.VMEM((rings, vecs, 128), f32),
            pltpu.VMEM((2, 128), f32),
        ),
        in_specs=[pl.BlockSpec(memory_space=pltpu.SMEM), anywhere, anywhere],
        out_specs=(vmem,) * 3,
        scratch_shapes=[
            pltpu.VMEM((LANCZOS, vecs, height + 2 * PAD, lanes), f32),
            pltpu.VMEM((LANCZOS, 2, vecs, height, lanes), f32),
            pltpu.VMEM((height, lanes), jnp.int32),
            pltpu.VMEM((height, lanes), f32),
            pltpu.VMEM((RING, vecs, 128), f32),
            pltpu.VMEM((2, vecs, 128), f32),
            dma((vecs + 1,)),
            dma((2,)),
            dma((2, 2, vecs, PARTS)),
            dma((2,)),
            dma((2,)),
            dma((2,)),
            pltpu.SemaphoreType.REGULAR(((count // 2).bit_length() - 1,)),
        ],
        compiler_params=pltpu.CompilerParams(
            collective_id=0, has_side_effects=True, vmem_limit_bytes=60 << 20
        ),
    )(energies, start_vectors, levels)
    return pl.pallas_call(
        finish,
        out_shape=(
            jax.ShapeDtypeStruct(start_vectors.shape, f32),
            jax.ShapeDtypeStruct((vecs, LANCZOS), f32),
            jax.ShapeDtypeStruct((vecs, LANCZOS - 1), f32),
            jax.ShapeDtypeStruct((vecs, 6), f32),
        ),
        in_specs=[vmem] * 3,
        out_specs=(anywhere, vmem, vmem, vmem),
        scratch_shapes=[pltpu.VMEM((vecs, height, lanes), f32), dma((vecs,))],
        compiler_params=pltpu.CompilerParams(vmem_limit_bytes=16 << 20),
    )(terms, parts, table)


def solution(mesh):
    in_specs = (P(None, "slab", None, None), P("slab", None, None), P())
    out_specs = (P(None, "slab", None, None), P(), P(), P())
    return jax.shard_map(
        functools.partial(shards, mesh.shape["slab"]),
        mesh=mesh, in_specs=in_specs, out_specs=out_specs, check_vma=False,
    )
```

```python
import functools

import jax
import jax.numpy as jnp
from jax import lax
from jax.experimental import pallas as pl
from jax.experimental.pallas import tpu as pltpu
from jax.sharding import PartitionSpec as P

LANCZOS = 8
RING = 16
PARTS = 8
PAD = 8
FAR = 64
RETURNED = 4
GAP = 12


def two_sum(a, b):
    s = a + b
    t = s - a
    return s, (a - (s - t)) + (b - t)


def quick(a, b):
    s = a + b
    return s, b - (s - a)


def add(x, y):
    s, e = two_sum(x[0], y[0])
    return quick(s, e + (x[1] + y[1]))


def wide(x):
    t = 4097.0 * x[0]
    upper = t - (t - x[0])
    return x[0], x[1], upper, x[0] - upper


def times(x, y):
    p = x[0] * y[0]
    e = ((x[2] * y[2] - p) + x[2] * y[3] + x[3] * y[2]) + x[3] * y[3]
    return p, e + (x[0] * y[1] + x[1] * y[0])


def minus(x, y):
    s, e = two_sum(x[0], -y[0])
    return s, e + (x[1] - y[1])


def twice(x):
    return tuple(2.0 * part for part in x)


def inverse(x):
    q = 1.0 / x[0]
    p, e = times(wide((q, 0.0 * q)), x)
    return wide(quick(q, q * ((1.0 - p) - e)))


def coefficients(dots):
    count = len(dots)
    norm = inverse(wide(dots[0]))
    nu = [wide((norm[0] * 0.0 + 1.0, norm[0] * 0.0)), wide(quick(*times(wide(dots[1]), norm)))]
    for k in range(2, count):
        nu.append(wide(quick(*minus(twice(times(wide(dots[k]), norm)), nu[k % 2]))))
    row, before, square = nu, None, None
    diag, offd = [], []
    for k in range(LANCZOS):
        inv = nu[0] if k == 0 else inverse(row[k])
        top = twice(row[1])[:2] if k == 0 else minus(row[k + 1], times(square, before[k]))
        alpha = wide(quick(*times(wide(quick(*top)), inv)))
        diag.append(0.5 * alpha[0])
        if k == LANCZOS - 1:
            break
        new = [None] * count
        for l in range(k + 1, count - 1 - k):
            s, e = two_sum(row[l + 1][0], row[l - 1][0])
            x = minus((s, e + (row[l + 1][1] + row[l - 1][1])), times(alpha, row[l]))
            new[l] = wide(quick(*(minus(x, times(square, before[l])) if k else x)))
        square = times(twice(new[1]) if k == 0 else new[k + 1], inv)
        square = wide(quick(*square))
        offd.append(0.5 * jnp.sqrt(square[0]))
        before, row = row, new
    return [x[0] for x in nu], diag, offd


def chebyshev(diag, offd, nu, centre, width):
    left = [None] + offd
    right = offd + [None]
    low, high = None, None
    for a, b, c in zip(diag, left, right):
        reach = b if c is None else c if b is None else b + c
        low = a - reach if low is None else jnp.minimum(low, a - reach)
        high = a + reach if high is None else jnp.maximum(high, a + reach)
    inv = 1.0 / (0.55 * (high - low))
    al = width * inv
    be = (centre - 0.5 * (high + low)) * inv
    p, q, r = 2.0 * be * be + al * al - 1.0, 4.0 * al * be, al * al
    first = [be, al]
    second = [p, q, r]
    third = [2.0 * be * p + al * q - be, 2.0 * be * q + al * (2.0 * p + r) - al, 2.0 * be * r + al * q, al * r]

    def dot(f, g):
        total = None
        for i, x in enumerate(f):
            for j, y in enumerate(g):
                term = (x * y) * (0.5 * (nu[i + j] + nu[abs(i - j)]))
                total = term if total is None else total + term
        return total

    start = [nu[0]]
    m1 = dot(start, first)
    moments = [
        m1,
        dot(start, second),
        dot(start, third),
        2.0 * dot(second, second) - 1.0,
        2.0 * dot(third, second) - m1,
        2.0 * dot(third, third) - 1.0,
    ]
    return third, moments


def kernel(
    count, energies, start, levels, terms, sums_out, table,
    field, halo, level, onsite, near_part, mine, scalars,
):
    vecs, rounds = start.shape[0], (count // 2).bit_length() - 1
    dma = pltpu.SemaphoreType.DMA
    body = functools.partial(
        steps, count, energies, start, levels, terms, sums_out, table,
        field, halo, level, onsite, near_part, mine, scalars,
    )
    pl.run_scoped(
        body, dma((vecs + 2,)), dma((2,)), dma((2, 2, vecs, PARTS)), dma((2,)), dma((2,)), dma((2,)),
        pltpu.SemaphoreType.REGULAR((rounds,)),
    )


def steps(
    count, energies, start, levels, terms, sums_out, table,
    field, halo, level, onsite, near_part, mine, scalars,
    load_sem, send_sem, recv_sem, last_sem, red_send, red_recv, known,
):
    me = lax.axis_index("slab")
    member = lax.rem(me, RING)
    ring = me // RING
    base = me - member
    rings = count // RING
    vecs, _, height, lanes = start.shape
    rows = height // PARTS
    mesh_id = pl.DeviceIdType.MESH

    def away(distance):
        return lax.rem(me + distance, count), lax.rem(me + count - distance, count)

    ahead, behind = away(1)

    def signal(sem, to):
        pl.semaphore_signal(sem, inc=1, device_id=(to,), device_id_type=mesh_id)

    barrier = pltpu.get_barrier_semaphore()
    for to in (ahead, behind):
        signal(barrier, to)
    loads = [
        pltpu.make_async_copy(start.at[v, 0], field.at[0, v, pl.ds(PAD, height)], load_sem.at[v]) for v in range(vecs)
    ]
    loads.append(pltpu.make_async_copy(levels.at[0], level, load_sem.at[vecs]))
    loads.append(pltpu.make_async_copy(energies, scalars, load_sem.at[vecs + 1]))
    for copy in loads:
        copy.start()

    def peer(i):
        return base + lax.rem(member + i, RING)

    def far(i):
        return lax.rem(me + i * RING, count)

    rounds = (count // 2).bit_length() - 1

    def spread(i):
        if i:
            pl.semaphore_wait(known.at[i - 1], 2)
        if i < rounds:
            for to in away(2**i):
                signal(known.at[i], to)

    def part_copy(k, v, h, side):
        to = ahead if side == 0 else behind
        at = h * rows
        sender = last_sem.at[side] if k == LANCZOS - 1 else send_sem.at[side]
        return pltpu.make_async_remote_copy(
            src_ref=field.at[k, v, pl.ds(PAD + at, rows)],
            dst_ref=halo.at[k, side, v, pl.ds(at, rows)],
            send_sem=sender, recv_sem=recv_sem.at[k % 2, side, v, h],
            device_id=(to,), device_id_type=mesh_id,
        )

    def sides(k, h):
        if k < LANCZOS - 1:
            return (0, 1)
        return (0,) if h < PARTS // 2 else (1,)

    def send(k, v, h):
        for side in sides(k, h):
            part_copy(k, v, h, side).start()

    pl.semaphore_wait(barrier, 2)
    for v in range(vecs):
        loads[v].wait()
        for h in range(PARTS):
            send(0, v, h)

    loads[vecs + 1].wait()
    values = [scalars[i] for i in range(energies.shape[0])]
    mean = sum(values[1:], values[0]) * (1.0 / len(values))
    spread_of = [(x - mean) * (x - mean) for x in values]
    spread_of = sum(spread_of[1:], spread_of[0]) * (1.0 / len(values))
    width = 2.0 * jnp.sqrt(jnp.full((1, 128), spread_of + 6.0, jnp.float32))
    inv_width = 1.0 / width
    inv_wide = jnp.concatenate([inv_width] * (lanes // 128), axis=1)
    table[0:1] = width
    table[1:2] = jnp.full((1, 128), mean, jnp.float32)

    loads[vecs].wait()
    for at in range(0, height, 64):
        ids = level[at : at + 64]
        energy = jnp.full(ids.shape, values[0] - mean, jnp.float32)
        for i in range(1, len(values)):
            energy = jnp.where(ids == i, values[i] - mean, energy)
        onsite[at : at + 64] = energy * inv_wide
    for v in range(vecs):
        field[0, v, 0:PAD] = field[0, v, height : height + PAD]
        field[0, v, PAD + height :] = field[0, v, PAD : 2 * PAD]
        terms[0, v] = field[0, v, PAD : PAD + height]

    def tile_sum(x):
        total = x[0:8]
        for i in range(8, rows, 8):
            total = total + x[i : i + 8]
        return total

    sums = {}

    def note(d, v, x):
        x = tile_sum(x)
        sums[d, v] = sums[d, v] + x if (d, v) in sums else x

    def unit(k, v, h):
        at = h * rows
        big = field[k, v, at : at + rows + 2 * PAD]
        deep = rows + 2 * PAD
        near = (pltpu.roll(big, 1, 0) + pltpu.roll(big, deep - 1, 0))[PAD : PAD + rows]
        here = big[PAD : PAD + rows]
        near = near + pltpu.roll(here, 1, 1) + pltpu.roll(here, lanes - 1, 1)
        for side in sides(k, h):
            part_copy(k, v, h, side).wait_recv()
        if k < LANCZOS - 1:
            near = near + (halo[k, 0, v, at : at + rows] + halo[k, 1, v, at : at + rows])
        else:
            near = near + 2.0 * halo[k, sides(k, h)[0], v, at : at + rows]
        new = onsite[at : at + rows] * here - inv_wide * near
        if k:
            new = 2.0 * new - field[k - 1, v, PAD + at : PAD + at + rows]
        if k < LANCZOS - 1:
            field[k + 1, v, PAD + at : PAD + at + rows] = new
            if h == 0:
                field[k + 1, v, PAD + height :] = new[0:PAD]
            if h == PARTS - 1:
                field[k + 1, v, 0:PAD] = new[rows - PAD :]
            send(k + 1, v, h)
        if k + 1 < RETURNED:
            terms[k + 1, v, at : at + rows] = new
        note(2 * k, v, here * here)
        note(2 * k + 1, v, here * new)

    lane = lax.broadcasted_iota(jnp.int32, (vecs, 128), 1)
    line = lax.broadcasted_iota(jnp.int32, (vecs, 128), 0)

    def gather(tile, k, v):
        for d in (2 * k, 2 * k + 1):
            whole = jnp.sum(jnp.sum(sums[d, v], axis=0, keepdims=True), axis=1, keepdims=True)
            tile = jnp.where((lane == d) & (line == v), whole, tile)
        return tile

    units = [(k, v, h) for k in range(LANCZOS) for v in range(vecs) for h in range(PARTS)]
    tile = jnp.zeros((vecs, 128), jnp.float32)
    turn = 0
    for i, (k, v, h) in enumerate(units):
        if i == turn * GAP and turn <= rounds:
            spread(turn)
            turn += 1
        unit(k, v, h)
        if h == PARTS - 1:
            tile = gather(tile, k, v)
    while turn <= rounds:
        spread(turn)
        turn += 1

    def exchange(leg, slots, index, size, target, tile):
        mine[leg] = tile
        slots[index] = tile

        for i in sorted(range(1, size), key=lambda i: abs(2 * i - size)):
            pltpu.make_async_remote_copy(
                src_ref=mine.at[leg], dst_ref=slots.at[index],
                send_sem=red_send.at[leg], recv_sem=red_recv.at[leg],
                device_id=(target(i),), device_id_type=mesh_id,
            ).start()

    def arrived(leg, slots, size):
        rest = slots.at[pl.ds(0, size - 1)]
        pltpu.make_async_copy(rest, rest, red_recv.at[leg]).wait()

    def sent(leg, slots, size):
        rest = slots.at[pl.ds(0, size - 1)]
        pltpu.make_async_copy(rest, rest, red_send.at[leg]).wait()

    exchange(0, near_part, member, RING, peer, tile)
    for side in range(2):
        whole = halo.at[pl.ds(0, LANCZOS - 1), 0]
        pltpu.make_async_copy(whole, whole, send_sem.at[side]).wait()
        half = halo.at[0, 0, pl.ds(0, vecs), pl.ds(0, height // 2)]
        pltpu.make_async_copy(half, half, last_sem.at[side]).wait()
    arrived(0, near_part, RING)
    pairs = [two_sum(near_part[i], near_part[i + 1]) for i in range(0, RING, 2)]
    while len(pairs) > 1:
        pairs = [add(x, y) for x, y in zip(pairs[::2], pairs[1::2])]
    high, low = pairs[0]
    tile = jnp.where(lane < FAR, high, pltpu.roll(low, FAR, 1))
    exchange(1, sums_out, ring, rings, far, tile)
    sent(0, near_part, RING)
    arrived(1, sums_out, rings)

    sent(1, sums_out, rings)


def finish(terms, parts, table, cheb, diag_out, offd_out, moments_out, result, diag_own, offd_own, moments_own, out_sem):
    _, vecs, height, lanes = terms.shape
    width, mean = table[0:1], table[1:2]
    pairs = []
    for i in range(parts.shape[0]):
        both = parts[i]
        pairs.append((both, pltpu.roll(both, FAR, 1)))
    while len(pairs) > 1:
        pairs = [add(x, y) for x, y in zip(pairs[::2], pairs[1::2])]
    high, low = pairs[0]

    def pick(x, d):
        return jnp.broadcast_to(x[:, d : d + 1], (vecs, 128))

    dots = [(pick(high, d), pick(low, d)) for d in range(2 * LANCZOS)]
    nu, diag, offd = coefficients(dots)
    diag = [width * a + mean for a in diag]
    offd = [width * b for b in offd]
    third, moments = chebyshev(diag, offd, nu, mean, width)

    copies = []

    def put(source, target):
        copies.append(pltpu.make_async_copy(source, target, out_sem.at[len(copies)]))
        copies[-1].start()

    for v in range(vecs):
        weights = [jnp.concatenate([x[v : v + 1]] * (lanes // 128), axis=1) for x in third]
        total = weights[0] * terms[0, v]
        for k in range(1, len(weights)):
            total = total + weights[k] * terms[k, v]
        result[v] = total
        put(result.at[v], cheb.at[v, 0])
    for own, ref, items in ((diag_own, diag_out, diag), (offd_own, offd_out, offd), (moments_own, moments_out, moments)):
        at = lax.broadcasted_iota(jnp.int32, own.shape, 1)
        value = jnp.zeros(own.shape, jnp.float32)
        for i, item in enumerate(items):
            value = jnp.where(at == i, item[:, : own.shape[1]], value)
        own[...] = value
        put(own, ref)
    for copy in copies:
        copy.wait()


def shards(count, start_vectors, levels, energies):
    vecs, _, height, lanes = start_vectors.shape
    rings = count // RING
    f32 = jnp.float32
    vmem = pl.BlockSpec(memory_space=pltpu.VMEM)
    anywhere = pl.BlockSpec(memory_space=pl.ANY)
    dma = pltpu.SemaphoreType.DMA
    terms, parts, table = pl.pallas_call(
        functools.partial(kernel, count),
        out_shape=(
            pltpu.VMEM((RETURNED, vecs, height, lanes), f32),
            pltpu.VMEM((rings, vecs, 128), f32),
            pltpu.VMEM((2, 128), f32),
        ),
        in_specs=[anywhere] * 3,
        out_specs=(vmem,) * 3,
        scratch_shapes=[
            pltpu.VMEM((LANCZOS, vecs, height + 2 * PAD, lanes), f32),
            pltpu.VMEM((LANCZOS, 2, vecs, height, lanes), f32),
            pltpu.VMEM((height, lanes), jnp.int32),
            pltpu.VMEM((height, lanes), f32),
            pltpu.VMEM((RING, vecs, 128), f32),
            pltpu.VMEM((2, vecs, 128), f32),
            pltpu.SMEM(energies.shape, f32),
        ],
        compiler_params=pltpu.CompilerParams(
            collective_id=0, has_side_effects=True, vmem_limit_bytes=60 << 20
        ),
    )(energies, start_vectors, levels)
    return pl.pallas_call(
        finish,
        out_shape=(
            jax.ShapeDtypeStruct(start_vectors.shape, f32),
            jax.ShapeDtypeStruct((vecs, LANCZOS), f32),
            jax.ShapeDtypeStruct((vecs, LANCZOS - 1), f32),
            jax.ShapeDtypeStruct((vecs, 6), f32),
        ),
        in_specs=[vmem] * 3,
        out_specs=(anywhere,) * 4,
        scratch_shapes=[
            pltpu.VMEM((vecs, height, lanes), f32),
            pltpu.VMEM((vecs, LANCZOS), f32),
            pltpu.VMEM((vecs, LANCZOS - 1), f32),
            pltpu.VMEM((vecs, 6), f32),
            dma((vecs + 3,)),
        ],
        compiler_params=pltpu.CompilerParams(vmem_limit_bytes=16 << 20),
    )(terms, parts, table)


def solution(mesh):
    in_specs = (P(None, "slab", None, None), P("slab", None, None), P())
    out_specs = (P(None, "slab", None, None), P(), P(), P())
    return jax.shard_map(
        functools.partial(shards, mesh.shape["slab"]),
        mesh=mesh, in_specs=in_specs, out_specs=out_specs, check_vma=False,
    )
```

```python
import functools

import jax
import jax.numpy as jnp
from jax import lax
from jax.experimental import pallas as pl
from jax.experimental.pallas import tpu as pltpu
from jax.sharding import PartitionSpec as P

LANCZOS = 8
RING = 16
PARTS = 8
PAD = 8
FAR = 64
RETURNED = 4
DIRECT = 13
GAP = 12


def two_sum(a, b):
    s = a + b
    t = s - a
    return s, (a - (s - t)) + (b - t)


def quick(a, b):
    s = a + b
    return s, b - (s - a)


def add(x, y):
    s, e = two_sum(x[0], y[0])
    return quick(s, e + (x[1] + y[1]))


def wide(x):
    t = 4097.0 * x[0]
    upper = t - (t - x[0])
    return x[0], x[1], upper, x[0] - upper


def times(x, y):
    p = x[0] * y[0]
    e = ((x[2] * y[2] - p) + x[2] * y[3] + x[3] * y[2]) + x[3] * y[3]
    return p, e + (x[0] * y[1] + x[1] * y[0])


def minus(x, y):
    s, e = two_sum(x[0], -y[0])
    return s, e + (x[1] - y[1])


def twice(x):
    return tuple(2.0 * part for part in x)


def inverse(x):
    q = 1.0 / x[0]
    p, e = times(wide((q, 0.0 * q)), x)
    return wide(quick(q, q * ((1.0 - p) - e)))


def coefficients(dots):
    count = len(dots)
    norm = inverse(wide(dots[0]))
    nu = [wide((norm[0] * 0.0 + 1.0, norm[0] * 0.0)), wide(quick(*times(wide(dots[1]), norm)))]
    for k in range(2, count):
        nu.append(wide(quick(*minus(twice(times(wide(dots[k]), norm)), nu[k % 2]))))
    row, before, square = nu, None, None
    diag, offd = [], []
    for k in range(LANCZOS):
        inv = nu[0] if k == 0 else inverse(row[k])
        top = twice(row[1])[:2] if k == 0 else minus(row[k + 1], times(square, before[k]))
        alpha = wide(quick(*times(wide(quick(*top)), inv)))
        diag.append(0.5 * alpha[0])
        if k == LANCZOS - 1:
            break
        new = [None] * count
        for l in range(k + 1, count - 1 - k):
            s, e = two_sum(row[l + 1][0], row[l - 1][0])
            x = minus((s, e + (row[l + 1][1] + row[l - 1][1])), times(alpha, row[l]))
            new[l] = wide(quick(*(minus(x, times(square, before[l])) if k else x)))
        square = times(twice(new[1]) if k == 0 else new[k + 1], inv)
        square = wide(quick(*square))
        offd.append(0.5 * jnp.sqrt(square[0]))
        before, row = row, new
    return [x[0] for x in nu], diag, offd


def chebyshev(diag, offd, nu, centre, width):
    left = [None] + offd
    right = offd + [None]
    low, high = None, None
    for a, b, c in zip(diag, left, right):
        reach = b if c is None else c if b is None else b + c
        low = a - reach if low is None else jnp.minimum(low, a - reach)
        high = a + reach if high is None else jnp.maximum(high, a + reach)
    inv = 1.0 / (0.55 * (high - low))
    al = width * inv
    be = (centre - 0.5 * (high + low)) * inv
    p, q, r = 2.0 * be * be + al * al - 1.0, 4.0 * al * be, al * al
    first = [be, al]
    second = [p, q, r]
    third = [2.0 * be * p + al * q - be, 2.0 * be * q + al * (2.0 * p + r) - al, 2.0 * be * r + al * q, al * r]

    def dot(f, g):
        total = None
        for i, x in enumerate(f):
            for j, y in enumerate(g):
                term = (x * y) * (0.5 * (nu[i + j] + nu[abs(i - j)]))
                total = term if total is None else total + term
        return total

    start = [nu[0]]
    m1 = dot(start, first)
    moments = [
        m1,
        dot(start, second),
        dot(start, third),
        2.0 * dot(second, second) - 1.0,
        2.0 * dot(third, second) - m1,
        2.0 * dot(third, third) - 1.0,
    ]
    return third, moments


def kernel(
    count, energies, start, levels, terms, sums_out, table,
    field, halo, level, onsite, near_part, mine, scalars,
):
    vecs, rounds = start.shape[0], (count // 2).bit_length() - 1
    dma = pltpu.SemaphoreType.DMA
    body = functools.partial(
        steps, count, energies, start, levels, terms, sums_out, table,
        field, halo, level, onsite, near_part, mine, scalars,
    )
    pl.run_scoped(
        body, dma((vecs + 2,)), dma((2,)), dma((3, 2, vecs, PARTS)), dma((2,)), dma((2,)), dma((2,)), dma((vecs,)),
        pltpu.SemaphoreType.REGULAR(()),
        pltpu.SemaphoreType.REGULAR((rounds,)),
    )


def steps(
    count, energies, start, levels, terms, sums_out, table,
    field, halo, level, onsite, near_part, mine, scalars,
    load_sem, send_sem, recv_sem, last_sem, red_send, red_recv, relay_sem, near_sem, known,
):
    me = lax.axis_index("slab")
    member = lax.rem(me, RING)
    ring = me // RING
    base = me - member
    rings = count // RING
    vecs, _, height, lanes = start.shape
    rows = height // PARTS
    mesh_id = pl.DeviceIdType.MESH

    def away(distance):
        return lax.rem(me + distance, count), lax.rem(me + count - distance, count)

    ahead, behind = away(1)

    def signal(sem, to):
        pl.semaphore_signal(sem, inc=1, device_id=(to,), device_id_type=mesh_id)

    relay = RING - 2
    is_first, is_last = (count - me) // count, (me + 1) // count

    def is_device(i):
        return (count - lax.rem(me + count - i, count)) // count

    is_relay = is_device(relay)
    before_relay, after_relay = is_device(relay - 1), is_device(relay + 1)

    barrier = pltpu.get_barrier_semaphore()

    @pl.when(before_relay == 0)
    def _():
        signal(barrier, ahead + is_last * (relay - ahead))

    @pl.when(after_relay == 0)
    def _():
        signal(barrier, behind)

    @pl.when(is_relay == 1)
    def _():
        signal(barrier, 0)

    loads = [
        pltpu.make_async_copy(start.at[v, 0], field.at[0, v, pl.ds(PAD, height)], load_sem.at[v]) for v in range(vecs)
    ]
    loads.append(pltpu.make_async_copy(levels.at[0], level, load_sem.at[vecs]))
    loads.append(pltpu.make_async_copy(energies, scalars, load_sem.at[vecs + 1]))
    for copy in loads:
        copy.start()

    def peer(i):
        return base + lax.rem(member + i, RING)

    def far(i):
        return lax.rem(me + i * RING, count)

    rounds = (count // 2).bit_length() - 1

    def spread(i):
        if i:
            pl.semaphore_wait(known.at[i - 1], 2)
        if i < rounds:
            for to in away(2**i):
                signal(known.at[i], to)

    def part_copy(k, v, h, side, leaving=False):
        to = ahead if side == 0 else behind
        slot, sem = k, k % 2
        if leaving and k == 0 and side == 1 and v * PARTS + h < DIRECT:
            to = to + is_first * (relay - to)
            slot, sem = is_first * LANCZOS, is_first * 2
        at = h * rows
        sender = last_sem.at[side] if k == LANCZOS - 1 else send_sem.at[side]
        return pltpu.make_async_remote_copy(
            src_ref=field.at[k, v, pl.ds(PAD + at, rows)],
            dst_ref=halo.at[slot, side, v, pl.ds(at, rows)],
            send_sem=sender, recv_sem=recv_sem.at[sem, side, v, h],
            device_id=(to,), device_id_type=mesh_id,
        )

    def sides(k, h):
        if k < LANCZOS - 1:
            return (0, 1)
        return (0,) if h < PARTS // 2 else (1,)

    def send(k, v, h):
        for side in sides(k, h):
            if k == 0 and side == 1 and v * PARTS + h >= DIRECT:
                pl.when(is_first == 0)(part_copy(k, v, h, side).start)
            else:
                part_copy(k, v, h, side, True).start()

    def send_rest():
        for i in range(DIRECT, vecs * PARTS):
            pl.when(is_first == 1)(part_copy(0, i // PARTS, i % PARTS, 1).start)

    @pl.when(is_relay == 0)
    def _():
        pl.semaphore_wait(barrier, 2)

    @pl.when(is_relay == 1)
    def _():
        pl.semaphore_wait(near_sem, 2)

    @pl.when(before_relay + after_relay == 1)
    def _():
        signal(near_sem, relay)

    for v in range(vecs):
        loads[v].wait()
        for h in range(PARTS):
            send(0, v, h)

    def forward(v, h):
        @pl.when(is_relay == 1)
        def _():
            if v + h == 0:
                pl.semaphore_wait(barrier, 1)
            part = halo.at[LANCZOS, 1, v, pl.ds(h * rows, rows)]
            pltpu.make_async_copy(part, part, recv_sem.at[2, 1, v, h]).wait()
            pltpu.make_async_remote_copy(
                src_ref=part, dst_ref=halo.at[0, 1, v, pl.ds(h * rows, rows)],
                send_sem=relay_sem.at[v], recv_sem=recv_sem.at[0, 1, v, h],
                device_id=(count - 1,), device_id_type=mesh_id,
            ).start()

    loads[vecs + 1].wait()
    values = [scalars[i] for i in range(energies.shape[0])]
    mean = sum(values[1:], values[0]) * (1.0 / len(values))
    spread_of = [(x - mean) * (x - mean) for x in values]
    spread_of = sum(spread_of[1:], spread_of[0]) * (1.0 / len(values))
    width = 2.0 * jnp.sqrt(jnp.full((1, 128), spread_of + 6.0, jnp.float32))
    inv_width = 1.0 / width
    inv_wide = jnp.concatenate([inv_width] * (lanes // 128), axis=1)
    table[0:1] = width
    table[1:2] = jnp.full((1, 128), mean, jnp.float32)

    loads[vecs].wait()
    for at in range(0, height, 64):
        ids = level[at : at + 64]
        energy = jnp.full(ids.shape, values[0] - mean, jnp.float32)
        for i in range(1, len(values)):
            energy = jnp.where(ids == i, values[i] - mean, energy)
        onsite[at : at + 64] = energy * inv_wide
    for v in range(vecs):
        field[0, v, 0:PAD] = field[0, v, height : height + PAD]
        field[0, v, PAD + height :] = field[0, v, PAD : 2 * PAD]
        terms[0, v] = field[0, v, PAD : PAD + height]

    def tile_sum(x):
        total = x[0:8]
        for i in range(8, rows, 8):
            total = total + x[i : i + 8]
        return total

    sums = {}

    def note(d, v, x):
        x = tile_sum(x)
        sums[d, v] = sums[d, v] + x if (d, v) in sums else x

    def unit(k, v, h):
        at = h * rows
        big = field[k, v, at : at + rows + 2 * PAD]
        deep = rows + 2 * PAD
        near = (pltpu.roll(big, 1, 0) + pltpu.roll(big, deep - 1, 0))[PAD : PAD + rows]
        here = big[PAD : PAD + rows]
        near = near + pltpu.roll(here, 1, 1) + pltpu.roll(here, lanes - 1, 1)
        for side in sides(k, h):
            part_copy(k, v, h, side).wait_recv()
        if k + v + h == 0:
            send_rest()
        if k < LANCZOS - 1:
            near = near + (halo[k, 0, v, at : at + rows] + halo[k, 1, v, at : at + rows])
        else:
            near = near + 2.0 * halo[k, sides(k, h)[0], v, at : at + rows]
        new = onsite[at : at + rows] * here - inv_wide * near
        if k:
            new = 2.0 * new - field[k - 1, v, PAD + at : PAD + at + rows]
        if k < LANCZOS - 1:
            field[k + 1, v, PAD + at : PAD + at + rows] = new
            if h == 0:
                field[k + 1, v, PAD + height :] = new[0:PAD]
            if h == PARTS - 1:
                field[k + 1, v, 0:PAD] = new[rows - PAD :]
            send(k + 1, v, h)
        if k + 1 < RETURNED:
            terms[k + 1, v, at : at + rows] = new
        note(2 * k, v, here * here)
        note(2 * k + 1, v, here * new)

    lane = lax.broadcasted_iota(jnp.int32, (vecs, 128), 1)
    line = lax.broadcasted_iota(jnp.int32, (vecs, 128), 0)

    def gather(tile, k, v):
        for d in (2 * k, 2 * k + 1):
            whole = jnp.sum(jnp.sum(sums[d, v], axis=0, keepdims=True), axis=1, keepdims=True)
            tile = jnp.where((lane == d) & (line == v), whole, tile)
        return tile

    units = [(k, v, h) for k in range(LANCZOS) for v in range(vecs) for h in range(PARTS)]
    tile = jnp.zeros((vecs, 128), jnp.float32)
    turn = 0
    for i, (k, v, h) in enumerate(units):
        if i == turn * GAP + 1 and turn <= rounds:
            spread(turn)
            turn += 1
        unit(k, v, h)
        if k == 1 and v * PARTS + h < DIRECT:
            forward(v, h)
        if h == PARTS - 1:
            tile = gather(tile, k, v)
    while turn <= rounds:
        spread(turn)
        turn += 1

    def exchange(leg, slots, index, size, target, tile):
        mine[leg] = tile
        slots[index] = tile

        for i in sorted(range(1, size), key=lambda i: abs(2 * i - size)):
            pltpu.make_async_remote_copy(
                src_ref=mine.at[leg], dst_ref=slots.at[index],
                send_sem=red_send.at[leg], recv_sem=red_recv.at[leg],
                device_id=(target(i),), device_id_type=mesh_id,
            ).start()

    def arrived(leg, slots, size):
        rest = slots.at[pl.ds(0, size - 1)]
        pltpu.make_async_copy(rest, rest, red_recv.at[leg]).wait()

    def sent(leg, slots, size):
        rest = slots.at[pl.ds(0, size - 1)]
        pltpu.make_async_copy(rest, rest, red_send.at[leg]).wait()

    exchange(0, near_part, member, RING, peer, tile)

    @pl.when(is_relay == 1)
    def _():
        for v in range(vecs):
            whole = halo.at[LANCZOS, 1, v, pl.ds(0, min(PARTS, DIRECT - v * PARTS) * rows)]
            pltpu.make_async_copy(whole, whole, relay_sem.at[v]).wait()

    for side in range(2):
        whole = halo.at[pl.ds(0, LANCZOS - 1), 0]
        pltpu.make_async_copy(whole, whole, send_sem.at[side]).wait()
        half = halo.at[0, 0, pl.ds(0, vecs), pl.ds(0, height // 2)]
        pltpu.make_async_copy(half, half, last_sem.at[side]).wait()
    arrived(0, near_part, RING)
    pairs = [two_sum(near_part[i], near_part[i + 1]) for i in range(0, RING, 2)]
    while len(pairs) > 1:
        pairs = [add(x, y) for x, y in zip(pairs[::2], pairs[1::2])]
    high, low = pairs[0]
    tile = jnp.where(lane < FAR, high, pltpu.roll(low, FAR, 1))
    exchange(1, sums_out, ring, rings, far, tile)
    sent(0, near_part, RING)
    arrived(1, sums_out, rings)

    sent(1, sums_out, rings)


def finish(terms, parts, table, cheb, diag_out, offd_out, moments_out, result, diag_own, offd_own, moments_own, out_sem):
    _, vecs, height, lanes = terms.shape
    width, mean = table[0:1], table[1:2]
    pairs = []
    for i in range(parts.shape[0]):
        both = parts[i]
        pairs.append((both, pltpu.roll(both, FAR, 1)))
    while len(pairs) > 1:
        pairs = [add(x, y) for x, y in zip(pairs[::2], pairs[1::2])]
    high, low = pairs[0]

    def pick(x, d):
        return jnp.broadcast_to(x[:, d : d + 1], (vecs, 128))

    dots = [(pick(high, d), pick(low, d)) for d in range(2 * LANCZOS)]
    nu, diag, offd = coefficients(dots)
    diag = [width * a + mean for a in diag]
    offd = [width * b for b in offd]
    third, moments = chebyshev(diag, offd, nu, mean, width)

    copies = []

    def put(source, target):
        copies.append(pltpu.make_async_copy(source, target, out_sem.at[len(copies)]))
        copies[-1].start()

    for v in range(vecs):
        weights = [jnp.concatenate([x[v : v + 1]] * (lanes // 128), axis=1) for x in third]
        total = weights[0] * terms[0, v]
        for k in range(1, len(weights)):
            total = total + weights[k] * terms[k, v]
        result[v] = total
        put(result.at[v], cheb.at[v, 0])
    for own, ref, items in ((diag_own, diag_out, diag), (offd_own, offd_out, offd), (moments_own, moments_out, moments)):
        at = lax.broadcasted_iota(jnp.int32, own.shape, 1)
        value = jnp.zeros(own.shape, jnp.float32)
        for i, item in enumerate(items):
            value = jnp.where(at == i, item[:, : own.shape[1]], value)
        own[...] = value
        put(own, ref)
    for copy in copies:
        copy.wait()


def shards(count, start_vectors, levels, energies):
    vecs, _, height, lanes = start_vectors.shape
    rings = count // RING
    f32 = jnp.float32
    vmem = pl.BlockSpec(memory_space=pltpu.VMEM)
    anywhere = pl.BlockSpec(memory_space=pl.ANY)
    dma = pltpu.SemaphoreType.DMA
    terms, parts, table = pl.pallas_call(
        functools.partial(kernel, count),
        out_shape=(
            pltpu.VMEM((RETURNED, vecs, height, lanes), f32),
            pltpu.VMEM((rings, vecs, 128), f32),
            pltpu.VMEM((2, 128), f32),
        ),
        in_specs=[anywhere] * 3,
        out_specs=(vmem,) * 3,
        scratch_shapes=[
            pltpu.VMEM((LANCZOS, vecs, height + 2 * PAD, lanes), f32),
            pltpu.VMEM((LANCZOS + 1, 2, vecs, height, lanes), f32),
            pltpu.VMEM((height, lanes), jnp.int32),
            pltpu.VMEM((height, lanes), f32),
            pltpu.VMEM((RING, vecs, 128), f32),
            pltpu.VMEM((2, vecs, 128), f32),
            pltpu.SMEM(energies.shape, f32),
        ],
        compiler_params=pltpu.CompilerParams(
            collective_id=0, has_side_effects=True, vmem_limit_bytes=60 << 20
        ),
    )(energies, start_vectors, levels)
    return pl.pallas_call(
        finish,
        out_shape=(
            jax.ShapeDtypeStruct(start_vectors.shape, f32),
            jax.ShapeDtypeStruct((vecs, LANCZOS), f32),
            jax.ShapeDtypeStruct((vecs, LANCZOS - 1), f32),
            jax.ShapeDtypeStruct((vecs, 6), f32),
        ),
        in_specs=[vmem] * 3,
        out_specs=(anywhere,) * 4,
        scratch_shapes=[
            pltpu.VMEM((vecs, height, lanes), f32),
            pltpu.VMEM((vecs, LANCZOS), f32),
            pltpu.VMEM((vecs, LANCZOS - 1), f32),
            pltpu.VMEM((vecs, 6), f32),
            dma((vecs + 3,)),
        ],
        compiler_params=pltpu.CompilerParams(vmem_limit_bytes=16 << 20),
    )(terms, parts, table)


def solution(mesh):
    in_specs = (P(None, "slab", None, None), P("slab", None, None), P())
    out_specs = (P(None, "slab", None, None), P(), P(), P())
    return jax.shard_map(
        functools.partial(shards, mesh.shape["slab"]),
        mesh=mesh, in_specs=in_specs, out_specs=out_specs, check_vma=False,
    )
```

```python
import functools

import jax
import jax.numpy as jnp
from jax import lax
from jax.experimental import pallas as pl
from jax.experimental.pallas import tpu as pltpu
from jax.sharding import PartitionSpec as P

LANCZOS = 8
RING = 16
PARTS = 16
PAD = 8
FAR = 64
RETURNED = 4
DIRECT = 26
GAP = 24


def two_sum(a, b):
    s = a + b
    t = s - a
    return s, (a - (s - t)) + (b - t)


def quick(a, b):
    s = a + b
    return s, b - (s - a)


def sum_up(items):
    rest = []
    while len(items) > 1:
        pairs = [two_sum(x, y) for x, y in zip(items[::2], items[1::2])]
        items = [s for s, _ in pairs]
        rest.extend(e for _, e in pairs)
    while len(rest) > 1:
        rest = [x + y for x, y in zip(rest[::2], rest[1::2])] + rest[len(rest) // 2 * 2 :]
    return items[0], rest[0]


def wide(x):
    t = 4097.0 * x[0]
    upper = t - (t - x[0])
    return x[0], x[1], upper, x[0] - upper


def times(x, y):
    p = x[0] * y[0]
    e = ((x[2] * y[2] - p) + x[2] * y[3] + x[3] * y[2]) + x[3] * y[3]
    return p, e + (x[0] * y[1] + x[1] * y[0])


def minus(x, y):
    s, e = two_sum(x[0], -y[0])
    return s, e + (x[1] - y[1])


def twice(x):
    return tuple(2.0 * part for part in x)


def inverse(x):
    q = 1.0 / x[0]
    p, e = times(wide((q, 0.0 * q)), x)
    return wide(quick(q, q * ((1.0 - p) - e)))


def coefficients(dots):
    count = len(dots)
    norm = inverse(wide(dots[0]))
    nu = [wide((norm[0] * 0.0 + 1.0, norm[0] * 0.0)), wide(quick(*times(wide(dots[1]), norm)))]
    for k in range(2, count):
        nu.append(wide(quick(*minus(twice(times(wide(dots[k]), norm)), nu[k % 2]))))
    row, before, square = nu, None, None
    diag, offd = [], []
    for k in range(LANCZOS):
        inv = nu[0] if k == 0 else inverse(row[k])
        top = twice(row[1])[:2] if k == 0 else minus(row[k + 1], times(square, before[k]))
        alpha = wide(quick(*times(wide(quick(*top)), inv)))
        diag.append(0.5 * alpha[0])
        if k == LANCZOS - 1:
            break
        new = [None] * count
        for l in range(k + 1, count - 1 - k):
            s, e = two_sum(row[l + 1][0], row[l - 1][0])
            x = minus((s, e + (row[l + 1][1] + row[l - 1][1])), times(alpha, row[l]))
            new[l] = wide(quick(*(minus(x, times(square, before[l])) if k else x)))
        square = times(twice(new[1]) if k == 0 else new[k + 1], inv)
        square = wide(quick(*square))
        offd.append(0.5 * jnp.sqrt(square[0]))
        before, row = row, new
    return [x[0] for x in nu], diag, offd


def chebyshev(diag, offd, nu, centre, width):
    left = [None] + offd
    right = offd + [None]
    low, high = None, None
    for a, b, c in zip(diag, left, right):
        reach = b if c is None else c if b is None else b + c
        low = a - reach if low is None else jnp.minimum(low, a - reach)
        high = a + reach if high is None else jnp.maximum(high, a + reach)
    inv = 1.0 / (0.55 * (high - low))
    al = width * inv
    be = (centre - 0.5 * (high + low)) * inv
    p, q, r = 2.0 * be * be + al * al - 1.0, 4.0 * al * be, al * al
    first = [be, al]
    second = [p, q, r]
    third = [2.0 * be * p + al * q - be, 2.0 * be * q + al * (2.0 * p + r) - al, 2.0 * be * r + al * q, al * r]

    def dot(f, g):
        total = None
        for i, x in enumerate(f):
            for j, y in enumerate(g):
                term = (x * y) * (0.5 * (nu[i + j] + nu[abs(i - j)]))
                total = term if total is None else total + term
        return total

    start = [nu[0]]
    m1 = dot(start, first)
    moments = [
        m1,
        dot(start, second),
        dot(start, third),
        2.0 * dot(second, second) - 1.0,
        2.0 * dot(third, second) - m1,
        2.0 * dot(third, third) - 1.0,
    ]
    return third, moments


def kernel(
    count, energies, start, levels, terms, sums_out, table,
    field, halo, level, onsite, near_part, mine, scalars,
):
    vecs, rounds = start.shape[0], (count // 2).bit_length() - 1
    dma = pltpu.SemaphoreType.DMA
    body = functools.partial(
        steps, count, energies, start, levels, terms, sums_out, table,
        field, halo, level, onsite, near_part, mine, scalars,
    )
    pl.run_scoped(
        body, dma((vecs + 2,)), dma((2,)), dma((3, 2, vecs, PARTS)), dma((2,)), dma((2,)), dma((2,)), dma((vecs,)),
        pltpu.SemaphoreType.REGULAR(()),
        pltpu.SemaphoreType.REGULAR((rounds,)),
    )


def steps(
    count, energies, start, levels, terms, sums_out, table,
    field, halo, level, onsite, near_part, mine, scalars,
    load_sem, send_sem, recv_sem, last_sem, red_send, red_recv, relay_sem, near_sem, known,
):
    me = lax.axis_index("slab")
    member = lax.rem(me, RING)
    ring = me // RING
    base = me - member
    rings = count // RING
    vecs, _, height, lanes = start.shape
    rows = height // PARTS
    mesh_id = pl.DeviceIdType.MESH

    def away(distance):
        return lax.rem(me + distance, count), lax.rem(me + count - distance, count)

    ahead, behind = away(1)

    def signal(sem, to):
        pl.semaphore_signal(sem, inc=1, device_id=(to,), device_id_type=mesh_id)

    relay = RING - 2
    is_first, is_last = (count - me) // count, (me + 1) // count

    def is_device(i):
        return (count - lax.rem(me + count - i, count)) // count

    is_relay = is_device(relay)
    before_relay, after_relay = is_device(relay - 1), is_device(relay + 1)

    barrier = pltpu.get_barrier_semaphore()

    @pl.when(before_relay == 0)
    def _():
        signal(barrier, ahead + is_last * (relay - ahead))

    @pl.when(after_relay == 0)
    def _():
        signal(barrier, behind)

    @pl.when(is_relay == 1)
    def _():
        signal(barrier, 0)

    loads = [
        pltpu.make_async_copy(start.at[v, 0], field.at[0, v, pl.ds(PAD, height)], load_sem.at[v]) for v in range(vecs)
    ]
    loads.append(pltpu.make_async_copy(levels.at[0], level, load_sem.at[vecs]))
    loads.append(pltpu.make_async_copy(energies, scalars, load_sem.at[vecs + 1]))
    for copy in loads:
        copy.start()

    def peer(i):
        return base + lax.rem(member + i, RING)

    def far(i):
        return lax.rem(me + i * RING, count)

    rounds = (count // 2).bit_length() - 1

    def spread(i):
        if i:
            pl.semaphore_wait(known.at[i - 1], 2)
        if i < rounds:
            for to in away(2**i):
                signal(known.at[i], to)

    def part_copy(k, v, h, side, leaving=False):
        to = ahead if side == 0 else behind
        slot, sem = k, k % 2
        if leaving and k == 0 and side == 1 and v * PARTS + h < DIRECT:
            to = to + is_first * (relay - to)
            slot, sem = is_first * LANCZOS, is_first * 2
        at = h * rows
        sender = last_sem.at[side] if k == LANCZOS - 1 else send_sem.at[side]
        return pltpu.make_async_remote_copy(
            src_ref=field.at[k, v, pl.ds(PAD + at, rows)],
            dst_ref=halo.at[slot, side, v, pl.ds(at, rows)],
            send_sem=sender, recv_sem=recv_sem.at[sem, side, v, h],
            device_id=(to,), device_id_type=mesh_id,
        )

    def sides(k, h):
        if k < LANCZOS - 1:
            return (0, 1)
        return (0,) if h < PARTS // 2 else (1,)

    def send(k, v, h):
        for side in sides(k, h):
            if k == 0 and side == 1 and v * PARTS + h >= DIRECT:
                pl.when(is_first == 0)(part_copy(k, v, h, side).start)
            else:
                part_copy(k, v, h, side, True).start()

    def send_rest():
        for i in range(DIRECT, vecs * PARTS):
            pl.when(is_first == 1)(part_copy(0, i // PARTS, i % PARTS, 1).start)

    @pl.when(is_relay == 0)
    def _():
        pl.semaphore_wait(barrier, 2)

    @pl.when(is_relay == 1)
    def _():
        pl.semaphore_wait(near_sem, 2)

    @pl.when(before_relay + after_relay == 1)
    def _():
        signal(near_sem, relay)

    for v in range(vecs):
        loads[v].wait()
        for h in range(PARTS):
            send(0, v, h)

    def forward(v, h):
        @pl.when(is_relay == 1)
        def _():
            if v + h == 0:
                pl.semaphore_wait(barrier, 1)
            part = halo.at[LANCZOS, 1, v, pl.ds(h * rows, rows)]
            pltpu.make_async_copy(part, part, recv_sem.at[2, 1, v, h]).wait()
            pltpu.make_async_remote_copy(
                src_ref=part, dst_ref=halo.at[0, 1, v, pl.ds(h * rows, rows)],
                send_sem=relay_sem.at[v], recv_sem=recv_sem.at[0, 1, v, h],
                device_id=(count - 1,), device_id_type=mesh_id,
            ).start()

    loads[vecs + 1].wait()
    values = [scalars[i] for i in range(energies.shape[0])]
    mean = sum(values[1:], values[0]) * (1.0 / len(values))
    spread_of = [(x - mean) * (x - mean) for x in values]
    spread_of = sum(spread_of[1:], spread_of[0]) * (1.0 / len(values))
    width = 2.0 * jnp.sqrt(jnp.full((1, 128), spread_of + 6.0, jnp.float32))
    inv_width = 1.0 / width
    inv_wide = jnp.concatenate([inv_width] * (lanes // 128), axis=1)
    table[0:1] = width
    table[1:2] = jnp.full((1, 128), mean, jnp.float32)

    loads[vecs].wait()
    for at in range(0, height, 64):
        ids = level[at : at + 64]
        energy = jnp.full(ids.shape, values[0] - mean, jnp.float32)
        for i in range(1, len(values)):
            energy = jnp.where(ids == i, values[i] - mean, energy)
        onsite[at : at + 64] = energy * inv_wide
    for v in range(vecs):
        field[0, v, 0:PAD] = field[0, v, height : height + PAD]
        field[0, v, PAD + height :] = field[0, v, PAD : 2 * PAD]
        terms[0, v] = field[0, v, PAD : PAD + height]

    def tile_sum(x):
        total = x[0:8]
        for i in range(8, rows, 8):
            total = total + x[i : i + 8]
        return total

    sums = {}

    def note(d, v, x):
        x = tile_sum(x)
        sums[d, v] = sums[d, v] + x if (d, v) in sums else x

    def unit(k, v, h):
        at = h * rows
        big = field[k, v, at : at + rows + 2 * PAD]
        deep = rows + 2 * PAD
        near = (pltpu.roll(big, 1, 0) + pltpu.roll(big, deep - 1, 0))[PAD : PAD + rows]
        here = big[PAD : PAD + rows]
        near = near + pltpu.roll(here, 1, 1) + pltpu.roll(here, lanes - 1, 1)
        for side in sides(k, h):
            part_copy(k, v, h, side).wait_recv()
        if k + v + h == 0:
            send_rest()
        if k < LANCZOS - 1:
            near = near + (halo[k, 0, v, at : at + rows] + halo[k, 1, v, at : at + rows])
        else:
            near = near + 2.0 * halo[k, sides(k, h)[0], v, at : at + rows]
        new = onsite[at : at + rows] * here - inv_wide * near
        if k:
            new = 2.0 * new - field[k - 1, v, PAD + at : PAD + at + rows]
        if k < LANCZOS - 1:
            field[k + 1, v, PAD + at : PAD + at + rows] = new
            if h == 0:
                field[k + 1, v, PAD + height :] = new[0:PAD]
            if h == PARTS - 1:
                field[k + 1, v, 0:PAD] = new[rows - PAD :]
            send(k + 1, v, h)
        if k + 1 < RETURNED:
            terms[k + 1, v, at : at + rows] = new
        note(2 * k, v, here * here)
        note(2 * k + 1, v, here * new)

    lane = lax.broadcasted_iota(jnp.int32, (1, 128), 1)

    def gather(tile, k, v):
        for d in (2 * k, 2 * k + 1):
            whole = jnp.sum(jnp.sum(sums[d, v], axis=0, keepdims=True), axis=1, keepdims=True)
            tile = jnp.where(lane == 2 * LANCZOS * v + d, whole, tile)
        return tile

    units = [(k, v, h) for k in range(LANCZOS) for v in range(vecs) for h in range(PARTS)]
    tile = jnp.zeros((1, 128), jnp.float32)
    turn = 0
    for i, (k, v, h) in enumerate(units):
        if i == turn * GAP + 1 and turn <= rounds:
            spread(turn)
            turn += 1
        unit(k, v, h)
        if k == 1 and v * PARTS + h < DIRECT:
            forward(v, h)
        if h == PARTS - 1:
            tile = gather(tile, k, v)
    while turn <= rounds:
        spread(turn)
        turn += 1

    def exchange(leg, slots, index, size, target, tile):
        mine[leg] = tile
        slots[index] = tile

        for i in sorted(range(1, size), key=lambda i: abs(2 * i - size)):
            pltpu.make_async_remote_copy(
                src_ref=mine.at[leg], dst_ref=slots.at[index],
                send_sem=red_send.at[leg], recv_sem=red_recv.at[leg],
                device_id=(target(i),), device_id_type=mesh_id,
            ).start()

    def arrived(leg, slots, size):
        rest = slots.at[pl.ds(0, size - 1)]
        pltpu.make_async_copy(rest, rest, red_recv.at[leg]).wait()

    def sent(leg, slots, size):
        rest = slots.at[pl.ds(0, size - 1)]
        pltpu.make_async_copy(rest, rest, red_send.at[leg]).wait()

    exchange(0, near_part, member, RING, peer, tile)

    @pl.when(is_relay == 1)
    def _():
        for v in range(vecs):
            whole = halo.at[LANCZOS, 1, v, pl.ds(0, min(PARTS, DIRECT - v * PARTS) * rows)]
            pltpu.make_async_copy(whole, whole, relay_sem.at[v]).wait()

    for side in range(2):
        whole = halo.at[pl.ds(0, LANCZOS - 1), 0]
        pltpu.make_async_copy(whole, whole, send_sem.at[side]).wait()
        half = halo.at[0, 0, pl.ds(0, vecs), pl.ds(0, height // 2)]
        pltpu.make_async_copy(half, half, last_sem.at[side]).wait()
    arrived(0, near_part, RING)
    high, low = sum_up([near_part[i] for i in range(RING)])
    tile = jnp.where(lane < FAR, high, pltpu.roll(low, FAR, 1))
    exchange(1, sums_out, ring, rings, far, tile)
    sent(0, near_part, RING)
    arrived(1, sums_out, rings)

    sent(1, sums_out, rings)


def finish(terms, parts, table, cheb, diag_out, offd_out, moments_out, result, diag_own, offd_own, moments_own, out_sem):
    _, vecs, height, lanes = terms.shape
    width, mean = table[0:1], table[1:2]
    both, rest = sum_up([parts[i] for i in range(parts.shape[0])])
    high = jnp.concatenate([pltpu.roll(both, (128 - 2 * LANCZOS * v) % 128, 1) if v else both for v in range(vecs)], axis=0)
    low = jnp.concatenate([pltpu.roll(both, FAR - 2 * LANCZOS * v, 1) for v in range(vecs)], axis=0)
    rest = jnp.concatenate([pltpu.roll(rest, 128 - 2 * LANCZOS * v, 1) if v else rest for v in range(vecs)], axis=0)
    high, low = quick(high, low + rest)

    def pick(x, d):
        return jnp.broadcast_to(x[:, d : d + 1], (vecs, 128))

    dots = [(pick(high, d), pick(low, d)) for d in range(2 * LANCZOS)]
    nu, diag, offd = coefficients(dots)
    diag = [width * a + mean for a in diag]
    offd = [width * b for b in offd]
    third, moments = chebyshev(diag, offd, nu, mean, width)

    copies = []

    def put(source, target):
        copies.append(pltpu.make_async_copy(source, target, out_sem.at[len(copies)]))
        copies[-1].start()

    for v in range(vecs):
        weights = [jnp.concatenate([x[v : v + 1]] * (lanes // 128), axis=1) for x in third]
        total = weights[0] * terms[0, v]
        for k in range(1, len(weights)):
            total = total + weights[k] * terms[k, v]
        result[v] = total
        put(result.at[v], cheb.at[v, 0])
    for own, ref, items in ((diag_own, diag_out, diag), (offd_own, offd_out, offd), (moments_own, moments_out, moments)):
        at = lax.broadcasted_iota(jnp.int32, own.shape, 1)
        value = jnp.zeros(own.shape, jnp.float32)
        for i, item in enumerate(items):
            value = jnp.where(at == i, item[:, : own.shape[1]], value)
        own[...] = value
        put(own, ref)
    for copy in copies:
        copy.wait()


def shards(count, start_vectors, levels, energies):
    vecs, _, height, lanes = start_vectors.shape
    rings = count // RING
    f32 = jnp.float32
    vmem = pl.BlockSpec(memory_space=pltpu.VMEM)
    anywhere = pl.BlockSpec(memory_space=pl.ANY)
    dma = pltpu.SemaphoreType.DMA
    terms, parts, table = pl.pallas_call(
        functools.partial(kernel, count),
        out_shape=(
            pltpu.VMEM((RETURNED, vecs, height, lanes), f32),
            pltpu.VMEM((rings, 1, 128), f32),
            pltpu.VMEM((2, 128), f32),
        ),
        in_specs=[anywhere] * 3,
        out_specs=(vmem,) * 3,
        scratch_shapes=[
            pltpu.VMEM((LANCZOS, vecs, height + 2 * PAD, lanes), f32),
            pltpu.VMEM((LANCZOS + 1, 2, vecs, height, lanes), f32),
            pltpu.VMEM((height, lanes), jnp.int32),
            pltpu.VMEM((height, lanes), f32),
            pltpu.VMEM((RING, 1, 128), f32),
            pltpu.VMEM((2, 1, 128), f32),
            pltpu.SMEM(energies.shape, f32),
        ],
        compiler_params=pltpu.CompilerParams(
            collective_id=0, has_side_effects=True, vmem_limit_bytes=60 << 20
        ),
    )(energies, start_vectors, levels)
    return pl.pallas_call(
        finish,
        out_shape=(
            jax.ShapeDtypeStruct(start_vectors.shape, f32),
            jax.ShapeDtypeStruct((vecs, LANCZOS), f32),
            jax.ShapeDtypeStruct((vecs, LANCZOS - 1), f32),
            jax.ShapeDtypeStruct((vecs, 6), f32),
        ),
        in_specs=[vmem] * 3,
        out_specs=(anywhere,) * 4,
        scratch_shapes=[
            pltpu.VMEM((vecs, height, lanes), f32),
            pltpu.VMEM((vecs, LANCZOS), f32),
            pltpu.VMEM((vecs, LANCZOS - 1), f32),
            pltpu.VMEM((vecs, 6), f32),
            dma((vecs + 3,)),
        ],
        compiler_params=pltpu.CompilerParams(vmem_limit_bytes=16 << 20),
    )(terms, parts, table)


def solution(mesh):
    in_specs = (P(None, "slab", None, None), P("slab", None, None), P())
    out_specs = (P(None, "slab", None, None), P(), P(), P())
    return jax.shard_map(
        functools.partial(shards, mesh.shape["slab"]),
        mesh=mesh, in_specs=in_specs, out_specs=out_specs, check_vma=False,
    )
```

```python
import functools

import jax
import jax.numpy as jnp
from jax import lax
from jax.experimental import pallas as pl
from jax.experimental.pallas import tpu as pltpu
from jax.sharding import PartitionSpec as P

LANCZOS = 8
RING = 16
PARTS = 16
PAD = 8
FAR = 64
RETURNED = 4
DIRECT = 24
GAP = 24


def two_sum(a, b):
    s = a + b
    t = s - a
    return s, (a - (s - t)) + (b - t)


def quick(a, b):
    s = a + b
    return s, b - (s - a)


def sum_up(items):
    rest = []
    while len(items) > 1:
        pairs = [two_sum(x, y) for x, y in zip(items[::2], items[1::2])]
        items = [s for s, _ in pairs]
        rest.extend(e for _, e in pairs)
    while len(rest) > 1:
        rest = [x + y for x, y in zip(rest[::2], rest[1::2])] + rest[len(rest) // 2 * 2 :]
    return items[0], rest[0]


def wide(x):
    t = 4097.0 * x[0]
    upper = t - (t - x[0])
    return x[0], x[1], upper, x[0] - upper


def times(x, y):
    p = x[0] * y[0]
    e = ((x[2] * y[2] - p) + x[2] * y[3] + x[3] * y[2]) + x[3] * y[3]
    return p, e + (x[0] * y[1] + x[1] * y[0])


def minus(x, y):
    s, e = two_sum(x[0], -y[0])
    return s, e + (x[1] - y[1])


def twice(x):
    return tuple(2.0 * part for part in x)


def inverse(x):
    q = 1.0 / x[0]
    p, e = times(wide((q, 0.0 * q)), x)
    return wide(quick(q, q * ((1.0 - p) - e)))


def coefficients(dots):
    count = len(dots)
    norm = inverse(wide(dots[0]))
    nu = [wide((norm[0] * 0.0 + 1.0, norm[0] * 0.0)), wide(quick(*times(wide(dots[1]), norm)))]
    for k in range(2, count):
        nu.append(wide(quick(*minus(twice(times(wide(dots[k]), norm)), nu[k % 2]))))
    row, before, square = nu, None, None
    diag, offd = [], []
    for k in range(LANCZOS):
        inv = nu[0] if k == 0 else inverse(row[k])
        top = twice(row[1])[:2] if k == 0 else minus(row[k + 1], times(square, before[k]))
        alpha = wide(quick(*times(wide(quick(*top)), inv)))
        diag.append(0.5 * alpha[0])
        if k == LANCZOS - 1:
            break
        new = [None] * count
        for l in range(k + 1, count - 1 - k):
            s, e = two_sum(row[l + 1][0], row[l - 1][0])
            x = minus((s, e + (row[l + 1][1] + row[l - 1][1])), times(alpha, row[l]))
            new[l] = wide(quick(*(minus(x, times(square, before[l])) if k else x)))
        square = times(twice(new[1]) if k == 0 else new[k + 1], inv)
        square = wide(quick(*square))
        offd.append(0.5 * jnp.sqrt(square[0]))
        before, row = row, new
    return [x[0] for x in nu], diag, offd


def chebyshev(diag, offd, nu, centre, width):
    left = [None] + offd
    right = offd + [None]
    low, high = None, None
    for a, b, c in zip(diag, left, right):
        reach = b if c is None else c if b is None else b + c
        low = a - reach if low is None else jnp.minimum(low, a - reach)
        high = a + reach if high is None else jnp.maximum(high, a + reach)
    inv = 1.0 / (0.55 * (high - low))
    al = width * inv
    be = (centre - 0.5 * (high + low)) * inv
    p, q, r = 2.0 * be * be + al * al - 1.0, 4.0 * al * be, al * al
    first = [be, al]
    second = [p, q, r]
    third = [2.0 * be * p + al * q - be, 2.0 * be * q + al * (2.0 * p + r) - al, 2.0 * be * r + al * q, al * r]

    def dot(f, g):
        total = None
        for i, x in enumerate(f):
            for j, y in enumerate(g):
                term = (x * y) * (0.5 * (nu[i + j] + nu[abs(i - j)]))
                total = term if total is None else total + term
        return total

    start = [nu[0]]
    m1 = dot(start, first)
    moments = [
        m1,
        dot(start, second),
        dot(start, third),
        2.0 * dot(second, second) - 1.0,
        2.0 * dot(third, second) - m1,
        2.0 * dot(third, third) - 1.0,
    ]
    return third, moments


def kernel(
    count, energies, start, levels, terms, sums_out, table,
    field, halo, level, onsite, near_part, mine, scalars,
):
    vecs, rounds = start.shape[0], (count // 2).bit_length() - 1
    dma = pltpu.SemaphoreType.DMA
    body = functools.partial(
        steps, count, energies, start, levels, terms, sums_out, table,
        field, halo, level, onsite, near_part, mine, scalars,
    )
    pl.run_scoped(
        body, dma((vecs + 2,)), dma((2,)), dma((3, 2, vecs, PARTS)), dma((2,)), dma((2,)), dma((2,)), dma((vecs,)),
        pltpu.SemaphoreType.REGULAR(()),
        pltpu.SemaphoreType.REGULAR((rounds,)),
    )


def steps(
    count, energies, start, levels, terms, sums_out, table,
    field, halo, level, onsite, near_part, mine, scalars,
    load_sem, send_sem, recv_sem, last_sem, red_send, red_recv, relay_sem, near_sem, known,
):
    me = lax.axis_index("slab")
    member = lax.rem(me, RING)
    ring = me // RING
    base = me - member
    rings = count // RING
    vecs, _, height, lanes = start.shape
    rows = height // PARTS
    mesh_id = pl.DeviceIdType.MESH

    def away(distance):
        return lax.rem(me + distance, count), lax.rem(me + count - distance, count)

    ahead, behind = away(1)

    def signal(sem, to):
        pl.semaphore_signal(sem, inc=1, device_id=(to,), device_id_type=mesh_id)

    relay = RING - 2
    is_first, is_last = (count - me) // count, (me + 1) // count

    def is_device(i):
        return (count - lax.rem(me + count - i, count)) // count

    is_relay = is_device(relay)
    before_relay, after_relay = is_device(relay - 1), is_device(relay + 1)

    barrier = pltpu.get_barrier_semaphore()

    @pl.when(before_relay == 0)
    def _():
        signal(barrier, ahead + is_last * (relay - ahead))

    @pl.when(after_relay == 0)
    def _():
        signal(barrier, behind)

    @pl.when(is_relay == 1)
    def _():
        signal(barrier, 0)

    loads = [
        pltpu.make_async_copy(start.at[v, 0], field.at[0, v, pl.ds(PAD, height)], load_sem.at[v]) for v in range(vecs)
    ]
    loads.append(pltpu.make_async_copy(levels.at[0], level, load_sem.at[vecs]))
    loads.append(pltpu.make_async_copy(energies, scalars, load_sem.at[vecs + 1]))
    for copy in loads:
        copy.start()

    def peer(i):
        return base + i

    def far(i):
        return i * RING + member

    rounds = (count // 2).bit_length() - 1

    def spread(i):
        if i:
            pl.semaphore_wait(known.at[i - 1], 2)
        if i < rounds:
            for to in away(2**i):
                signal(known.at[i], to)

    def part_copy(k, v, h, side, leaving=False):
        to = ahead if side == 0 else behind
        slot, sem = k, k % 2
        if leaving and k == 0 and side == 1 and v * PARTS + h < DIRECT:
            to = to + is_first * (relay - to)
            slot, sem = is_first * LANCZOS, is_first * 2
        at = h * rows
        sender = last_sem.at[side] if k == LANCZOS - 1 else send_sem.at[side]
        return pltpu.make_async_remote_copy(
            src_ref=field.at[k, v, pl.ds(PAD + at, rows)],
            dst_ref=halo.at[slot, side, v, pl.ds(at, rows)],
            send_sem=sender, recv_sem=recv_sem.at[sem, side, v, h],
            device_id=(to,), device_id_type=mesh_id,
        )

    def sides(k, h):
        if k < LANCZOS - 1:
            return (0, 1)
        return (0,) if h < PARTS // 2 else (1,)

    def send(k, v, h):
        for side in sides(k, h):
            if k == 0 and side == 1 and v * PARTS + h >= DIRECT:
                pl.when(is_first == 0)(part_copy(k, v, h, side).start)
            else:
                part_copy(k, v, h, side, True).start()

    def send_rest():
        for i in range(DIRECT, vecs * PARTS):
            pl.when(is_first == 1)(part_copy(0, i // PARTS, i % PARTS, 1).start)

    @pl.when(is_relay == 0)
    def _():
        pl.semaphore_wait(barrier, 2)

    @pl.when(is_relay == 1)
    def _():
        pl.semaphore_wait(near_sem, 2)

    @pl.when(before_relay + after_relay == 1)
    def _():
        signal(near_sem, relay)

    for v in range(vecs):
        loads[v].wait()
        for h in range(PARTS):
            send(0, v, h)

    def forward(v, h):
        @pl.when(is_relay == 1)
        def _():
            if v + h == 0:
                pl.semaphore_wait(barrier, 1)
            part = halo.at[LANCZOS, 1, v, pl.ds(h * rows, rows)]
            pltpu.make_async_copy(part, part, recv_sem.at[2, 1, v, h]).wait()
            pltpu.make_async_remote_copy(
                src_ref=part, dst_ref=halo.at[0, 1, v, pl.ds(h * rows, rows)],
                send_sem=relay_sem.at[v], recv_sem=recv_sem.at[0, 1, v, h],
                device_id=(count - 1,), device_id_type=mesh_id,
            ).start()

    loads[vecs + 1].wait()
    values = [scalars[i] for i in range(energies.shape[0])]
    mean = sum(values[1:], values[0]) * (1.0 / len(values))
    spread_of = [(x - mean) * (x - mean) for x in values]
    spread_of = sum(spread_of[1:], spread_of[0]) * (1.0 / len(values))
    width = 2.0 * jnp.sqrt(jnp.full((1, 128), spread_of + 6.0, jnp.float32))
    inv_width = 1.0 / width
    inv_wide = jnp.concatenate([inv_width] * (lanes // 128), axis=1)
    table[0:1] = width
    table[1:2] = jnp.full((1, 128), mean, jnp.float32)

    loads[vecs].wait()
    for at in range(0, height, 64):
        ids = level[at : at + 64]
        energy = jnp.full(ids.shape, values[0] - mean, jnp.float32)
        for i in range(1, len(values)):
            energy = jnp.where(ids == i, values[i] - mean, energy)
        onsite[at : at + 64] = energy * inv_wide
    for v in range(vecs):
        field[0, v, 0:PAD] = field[0, v, height : height + PAD]
        field[0, v, PAD + height :] = field[0, v, PAD : 2 * PAD]
        terms[0, v] = field[0, v, PAD : PAD + height]

    def tile_sum(x):
        total = x[0:8]
        for i in range(8, rows, 8):
            total = total + x[i : i + 8]
        return total

    sums = {}

    def note(d, v, x):
        x = tile_sum(x)
        sums[d, v] = sums[d, v] + x if (d, v) in sums else x

    def unit(k, v, h):
        at = h * rows
        big = field[k, v, at : at + rows + 2 * PAD]
        deep = rows + 2 * PAD
        near = (pltpu.roll(big, 1, 0) + pltpu.roll(big, deep - 1, 0))[PAD : PAD + rows]
        here = big[PAD : PAD + rows]
        near = near + pltpu.roll(here, 1, 1) + pltpu.roll(here, lanes - 1, 1)
        for side in sides(k, h):
            part_copy(k, v, h, side).wait_recv()
        if k + v + h == 0:
            send_rest()
        if k < LANCZOS - 1:
            near = near + (halo[k, 0, v, at : at + rows] + halo[k, 1, v, at : at + rows])
        else:
            near = near + 2.0 * halo[k, sides(k, h)[0], v, at : at + rows]
        new = onsite[at : at + rows] * here - inv_wide * near
        if k:
            new = 2.0 * new - field[k - 1, v, PAD + at : PAD + at + rows]
        if k < LANCZOS - 1:
            field[k + 1, v, PAD + at : PAD + at + rows] = new
            if h == 0:
                field[k + 1, v, PAD + height :] = new[0:PAD]
            if h == PARTS - 1:
                field[k + 1, v, 0:PAD] = new[rows - PAD :]
            send(k + 1, v, h)
        if k + 1 < RETURNED:
            terms[k + 1, v, at : at + rows] = new
        note(2 * k, v, here * here)
        note(2 * k + 1, v, here * new)

    lane = lax.broadcasted_iota(jnp.int32, (1, 128), 1)

    def gather(tile, k, v):
        for d in (2 * k, 2 * k + 1):
            whole = jnp.sum(jnp.sum(sums[d, v], axis=0, keepdims=True), axis=1, keepdims=True)
            tile = jnp.where(lane == 2 * LANCZOS * v + d, whole, tile)
        return tile

    units = [(k, v, h) for k in range(LANCZOS) for v in range(vecs) for h in range(PARTS)]
    tile = jnp.zeros((1, 128), jnp.float32)
    turn = 0
    for i, (k, v, h) in enumerate(units):
        if i == turn * GAP + 1 and turn <= rounds:
            spread(turn)
            turn += 1
        unit(k, v, h)
        if k == 1 and v * PARTS + h < DIRECT:
            forward(v, h)
        if h == PARTS - 1:
            tile = gather(tile, k, v)
    while turn <= rounds:
        spread(turn)
        turn += 1

    def exchange(leg, slots, index, size, target, tile):
        mine[leg] = tile
        slots[index] = tile

        for i in range(size - 1):
            pltpu.make_async_remote_copy(
                src_ref=mine.at[leg], dst_ref=slots.at[index],
                send_sem=red_send.at[leg], recv_sem=red_recv.at[leg],
                device_id=(target(i + (i + size - index) // size),), device_id_type=mesh_id,
            ).start()

    def arrived(leg, slots, size):
        rest = slots.at[pl.ds(0, size - 1)]
        pltpu.make_async_copy(rest, rest, red_recv.at[leg]).wait()

    def sent(leg, slots, size):
        rest = slots.at[pl.ds(0, size - 1)]
        pltpu.make_async_copy(rest, rest, red_send.at[leg]).wait()

    exchange(0, near_part, member, RING, peer, tile)

    @pl.when(is_relay == 1)
    def _():
        for v in range(vecs):
            whole = halo.at[LANCZOS, 1, v, pl.ds(0, min(PARTS, DIRECT - v * PARTS) * rows)]
            pltpu.make_async_copy(whole, whole, relay_sem.at[v]).wait()

    for side in range(2):
        whole = halo.at[pl.ds(0, LANCZOS - 1), 0]
        pltpu.make_async_copy(whole, whole, send_sem.at[side]).wait()
        half = halo.at[0, 0, pl.ds(0, vecs), pl.ds(0, height // 2)]
        pltpu.make_async_copy(half, half, last_sem.at[side]).wait()
    arrived(0, near_part, RING)
    high, low = sum_up([near_part[i] for i in range(RING)])
    tile = jnp.where(lane < FAR, high, pltpu.roll(low, FAR, 1))
    exchange(1, sums_out, ring, rings, far, tile)
    sent(0, near_part, RING)
    arrived(1, sums_out, rings)

    sent(1, sums_out, rings)


def finish(terms, parts, table, cheb, diag_out, offd_out, moments_out, result, diag_own, offd_own, moments_own, out_sem):
    _, vecs, height, lanes = terms.shape
    width, mean = table[0:1], table[1:2]
    both, rest = sum_up([parts[i] for i in range(parts.shape[0])])
    high = jnp.concatenate([pltpu.roll(both, (128 - 2 * LANCZOS * v) % 128, 1) if v else both for v in range(vecs)], axis=0)
    low = jnp.concatenate([pltpu.roll(both, FAR - 2 * LANCZOS * v, 1) for v in range(vecs)], axis=0)
    rest = jnp.concatenate([pltpu.roll(rest, 128 - 2 * LANCZOS * v, 1) if v else rest for v in range(vecs)], axis=0)
    high, low = quick(high, low + rest)

    def pick(x, d):
        return jnp.broadcast_to(x[:, d : d + 1], (vecs, 128))

    dots = [(pick(high, d), pick(low, d)) for d in range(2 * LANCZOS)]
    nu, diag, offd = coefficients(dots)
    diag = [width * a + mean for a in diag]
    offd = [width * b for b in offd]
    third, moments = chebyshev(diag, offd, nu, mean, width)

    copies = []

    def put(source, target):
        copies.append(pltpu.make_async_copy(source, target, out_sem.at[len(copies)]))
        copies[-1].start()

    for v in range(vecs):
        weights = [jnp.concatenate([x[v : v + 1]] * (lanes // 128), axis=1) for x in third]
        total = weights[0] * terms[0, v]
        for k in range(1, len(weights)):
            total = total + weights[k] * terms[k, v]
        result[v] = total
        put(result.at[v], cheb.at[v, 0])
    for own, ref, items in ((diag_own, diag_out, diag), (offd_own, offd_out, offd), (moments_own, moments_out, moments)):
        at = lax.broadcasted_iota(jnp.int32, own.shape, 1)
        value = jnp.zeros(own.shape, jnp.float32)
        for i, item in enumerate(items):
            value = jnp.where(at == i, item[:, : own.shape[1]], value)
        own[...] = value
        put(own, ref)
    for copy in copies:
        copy.wait()


def shards(count, start_vectors, levels, energies):
    vecs, _, height, lanes = start_vectors.shape
    rings = count // RING
    f32 = jnp.float32
    vmem = pl.BlockSpec(memory_space=pltpu.VMEM)
    anywhere = pl.BlockSpec(memory_space=pl.ANY)
    dma = pltpu.SemaphoreType.DMA
    terms, parts, table = pl.pallas_call(
        functools.partial(kernel, count),
        out_shape=(
            pltpu.VMEM((RETURNED, vecs, height, lanes), f32),
            pltpu.VMEM((rings, 1, 128), f32),
            pltpu.VMEM((2, 128), f32),
        ),
        in_specs=[anywhere] * 3,
        out_specs=(vmem,) * 3,
        scratch_shapes=[
            pltpu.VMEM((LANCZOS, vecs, height + 2 * PAD, lanes), f32),
            pltpu.VMEM((LANCZOS + 1, 2, vecs, height, lanes), f32),
            pltpu.VMEM((height, lanes), jnp.int32),
            pltpu.VMEM((height, lanes), f32),
            pltpu.VMEM((RING, 1, 128), f32),
            pltpu.VMEM((2, 1, 128), f32),
            pltpu.SMEM(energies.shape, f32),
        ],
        compiler_params=pltpu.CompilerParams(
            collective_id=0, has_side_effects=True, vmem_limit_bytes=60 << 20
        ),
    )(energies, start_vectors, levels)
    return pl.pallas_call(
        finish,
        out_shape=(
            jax.ShapeDtypeStruct(start_vectors.shape, f32),
            jax.ShapeDtypeStruct((vecs, LANCZOS), f32),
            jax.ShapeDtypeStruct((vecs, LANCZOS - 1), f32),
            jax.ShapeDtypeStruct((vecs, 6), f32),
        ),
        in_specs=[vmem] * 3,
        out_specs=(anywhere,) * 4,
        scratch_shapes=[
            pltpu.VMEM((vecs, height, lanes), f32),
            pltpu.VMEM((vecs, LANCZOS), f32),
            pltpu.VMEM((vecs, LANCZOS - 1), f32),
            pltpu.VMEM((vecs, 6), f32),
            dma((vecs + 3,)),
        ],
        compiler_params=pltpu.CompilerParams(vmem_limit_bytes=16 << 20),
    )(terms, parts, table)


def solution(mesh):
    in_specs = (P(None, "slab", None, None), P("slab", None, None), P())
    out_specs = (P(None, "slab", None, None), P(), P(), P())
    return jax.shard_map(
        functools.partial(shards, mesh.shape["slab"]),
        mesh=mesh, in_specs=in_specs, out_specs=out_specs, check_vma=False,
    )
```
